32 devices in a mesh: src: 4 (over y, x), rcv: 8 (over z, core).
Axes of the slice: x: 2, y: 2, z: 4, core: 2. Of those that a mesh axis runs over, the one named last changes fastest.
Arguments:
- wavefield: float32 [2, 16, 2048, 2048], P(None, None, 'rcv', 'src')
- surface_band: float32 [2, 2048, 1024], P(None, 'rcv'), may hold values from -0.75 to 0.75
- band_shift: int32 [32], P('rcv'), may hold values from -16 to 16
- trace_mask: int32 [2048], P('rcv'), may hold values 0 or 1
- shot_taper: float32 [5], replicated, may hold values from 0.2 to 1
Outputs:
- multiples: float32 [2, 16, 2048, 2048], P(None, None, 'rcv', 'src')
- primaries: float32 [2, 16, 2048, 2048], P(None, None, 'rcv', 'src')
The draws below stay inside these ranges and needn't reach their ends.
All inputs are finite; a program needn't handle non-finite values. No bound on the sum of `trace_mask` on one device may be relied on, other than what follows from the above.
Results may differ from the reference program's by a relative error of at most 0.0003.
Values sent between devices are 32-bit elements; how exact they have to be, the bound alone decides.
A program may use at most 192 MiB of HBM per device.

```python
import jax
import jax.numpy as jnp
from jax import lax

F = 16
NS = 2048
NR = 2048
APER = 64
SHIFT = 16
BLOCK = 64
SHALF = 2


def draw_wavefield(key, part):
    base_key = jax.random.fold_in(key, 7)
    noise_key, row_key, col_key = jax.random.split(base_key, 3)
    rows = jnp.exp(jax.random.uniform(row_key, (NS,), jnp.float32, -1.15, 1.15)) * jnp.exp(1.0986 * (jnp.arange(NS, dtype=jnp.float32) / NS - 0.5))
    cols = jnp.exp(jax.random.uniform(col_key, (NR,), jnp.float32, -1.15, 1.15)) * jnp.exp(1.0986 * (jnp.arange(NR, dtype=jnp.float32) / NR - 0.5))
    noise = jax.random.normal(noise_key, (2, F, NR, NS), jnp.float32)
    return noise * cols[None, None, :, None] * rows[None, None, None, :] * 0.5


def touch_ends(array, key, least, largest):
    place = [jax.random.randint(jax.random.fold_in(key, axis), (), 0, length) for axis, length in enumerate(array.shape)]
    longest = array.shape.index(max(array.shape))
    neighbour = place[:longest] + [(place[longest] + 1) % array.shape[longest]] + place[longest + 1:]
    return array.at[tuple(place)].set(least).at[tuple(neighbour)].set(largest)


def levels(stream_key, extent, cuts, low, top_value):
    level, own = 1.0, jax.random.fold_in(stream_key, 6)
    for position, shards_of in cuts:
        heights = jnp.exp(jax.random.uniform(jax.random.fold_in(own, position), (shards_of,), jnp.float32, low / len(cuts), top_value / len(cuts)))
        level = level * jnp.repeat(heights, extent[position] // shards_of).reshape([-1 if axis == position else 1 for axis in range(len(extent))])
    return level


def gaussian(stream_key, extent, spread, limit, shards=(), kind=jnp.bfloat16):
    level = levels(stream_key, extent, shards, -0.22, 0.18) if shards else 1.0
    drawn = jax.random.normal(stream_key, extent, jnp.float32) * spread * level
    return jnp.minimum(jnp.maximum(drawn, -limit), limit).astype(kind)


def setup_inputs(seed: int = 0) -> dict:
    key_of = jax.random.split(jax.random.key(seed), 6)
    wavefield = draw_wavefield(jax.random.fold_in(key_of[5], 71), 0)
    surface_band = gaussian(key_of[1], (2, NR, F * APER), APER ** -0.5, 0.75, ((1, 8),), jnp.float32)
    band_shift = touch_ends(jax.random.randint(key_of[2], (NR // BLOCK,), -SHIFT, SHIFT + 1), jax.random.fold_in(key_of[2], 1), -SHIFT, SHIFT).astype(jnp.int32)
    trace_mask = touch_ends((jax.random.randint(key_of[3], (NR,), 0, 8) < 7).astype(jnp.int32), jax.random.fold_in(key_of[3], 1), 0, 1)
    shot_taper = jnp.clip(jax.random.uniform(key_of[4], (2 * SHALF + 1,), jnp.float32, 0.2, 1.0), 0.2, 1.0)
    return dict(wavefield=wavefield, surface_band=surface_band, band_shift=band_shift, trace_mask=trace_mask, shot_taper=shot_taper)


def band_matrix(band_piece):
    columns = band_piece.shape[3]
    taps = band_piece.shape[2]
    rows_index = jnp.arange(columns + taps - 1, dtype=jnp.int32)
    cols_index = jnp.arange(columns, dtype=jnp.int32)
    tap_index = jnp.arange(taps, dtype=jnp.int32)
    onehot = (tap_index[:, None, None] == rows_index[None, :, None] - cols_index[None, None, :]).astype(jnp.float32)
    return jnp.einsum('xftc,tjc->xfjc', band_piece, onehot, precision=lax.Precision.HIGHEST)

def complex_product(window, band):
    real_part = jnp.einsum('fjc,fjs->fcs', band[0], window[0], precision=lax.Precision.HIGHEST) - jnp.einsum('fjc,fjs->fcs', band[1], window[1], precision=lax.Precision.HIGHEST)
    imag_part = jnp.einsum('fjc,fjs->fcs', band[1], window[0], precision=lax.Precision.HIGHEST) + jnp.einsum('fjc,fjs->fcs', band[0], window[1], precision=lax.Precision.HIGHEST)
    return jnp.stack([real_part, imag_part])

def reference(wavefield, surface_band, band_shift, trace_mask, shot_taper):
    masked = wavefield * trace_mask.astype(jnp.float32)[None, None, :, None]
    halo_width = APER // 2 + SHIFT
    padded = jnp.pad(masked, ((0, 0), (0, 0), (halo_width, halo_width), (0, 0)))
    band_full = jnp.transpose(surface_band.reshape(2, NR, F, APER), (0, 2, 3, 1))

    def one_block(index):
        start = index * BLOCK + halo_width - APER // 2 + band_shift[index]
        window = lax.dynamic_slice_in_dim(padded, start.astype(jnp.int32), BLOCK + APER - 1, 2)
        band_piece = lax.dynamic_slice_in_dim(band_full, (index * BLOCK).astype(jnp.int32), BLOCK, 3)
        return complex_product(window, band_matrix(band_piece))
    stacked = lax.map(one_block, jnp.arange(NR // BLOCK, dtype=jnp.int32))
    predicted = jnp.moveaxis(stacked, 0, 2).reshape(2, F, NR, NS)
    shot_padded = jnp.pad(predicted, ((0, 0), (0, 0), (0, 0), (SHALF, SHALF)))
    multiples = jnp.zeros_like(predicted)
    for offset_row in range(2 * SHALF + 1):
        multiples = multiples + shot_taper[offset_row] * shot_padded[:, :, :, offset_row:offset_row + NS]
    data_energy = lax.optimization_barrier(jnp.sum(wavefield * wavefield, axis=(0, 2, 3)))
    pred_energy = lax.optimization_barrier(jnp.sum(multiples * multiples, axis=(0, 2, 3)))
    gain = jnp.sqrt((data_energy + 1e-06) / (pred_energy + 1e-06))
    primaries = wavefield - gain[None, :, None, None] * multiples
    return (multiples, primaries)
```

```python
import functools

import jax
import jax.numpy as jnp
from jax import lax
from jax.experimental import pallas as pl
from jax.experimental.pallas import tpu as pltpu
from jax.sharding import PartitionSpec as P

APER = 64
SHIFT = 16
BLOCK = 64
HALF = BLOCK // 2
SHALF = 2
LANES = 128
DEPTH = 128
HALO = APER // 2 + SHIFT
FIRST = 2
STRIP = 16
SLOTS = 8
MESH = pl.DeviceIdType.MESH


def split(cells):
    high = cells.astype(jnp.bfloat16)
    low = (cells - high.astype(jnp.float32)).astype(jnp.bfloat16)
    return high, low


def forward_kernel(axes, shift_ref, taper_ref, mask_ref, wave_hbm, band_hbm, *refs):
    wave_ref, mult_ref, gain_ref = refs[:3]
    (
        band_ref, weight_ref, turn_ref, high_ref, low_ref, above_ref, below_ref, edge_ref, next_ref, prev_ref, corner_ref, masks_ref,
        data_ref, pred_ref, mine_ref, plane_ref, space_ref,
        load_sem, band_sem, send_up, recv_up, send_down, recv_down, send_mask, recv_mask,
        send_edge, recv_edge, send_corner, recv_corner, own_sem, send_a, recv_a, send_b, recv_b,
    ) = refs[3:]
    (slow, slow_count), (fast, fast_count) = axes
    slow_me, fast_me = lax.axis_index(slow), lax.axis_index(fast)
    _, slices, receivers, shots = wave_ref.shape
    blocks = receivers // BLOCK
    has_above, has_below = fast_me > 0, fast_me < fast_count - 1
    has_prev, has_next = slow_me > 0, slow_me < slow_count - 1

    def slow_peer(d):
        return {slow: lax.rem(slow_me + d, slow_count)}

    def fast_peer(d):
        return {fast: lax.rem(fast_me + d, fast_count)}

    corners = []
    for i, (down, right) in enumerate([(1, 1), (1, -1), (-1, 1), (-1, -1)]):
        there = (has_below if down > 0 else has_above) & (has_next if right > 0 else has_prev)
        came = (has_above if down > 0 else has_below) & (has_prev if right > 0 else has_next)
        peer = {fast: fast_me + down, slow: slow_me + right}
        rows = pl.ds(receivers - HALO if down > 0 else 0, HALO)
        corners.append((i, there, came, peer, rows))

    def load(f):
        return pltpu.make_async_copy(wave_hbm.at[:, f], wave_ref.at[:, f], load_sem.at[f])

    def up(f):
        return pltpu.make_async_remote_copy(
            src_ref=wave_hbm.at[:, f, pl.ds(receivers - HALO, HALO)], dst_ref=above_ref.at[f],
            send_sem=send_up.at[f], recv_sem=recv_up.at[f],
            device_id={fast: fast_me + 1}, device_id_type=MESH,
        )

    def down(f):
        return pltpu.make_async_remote_copy(
            src_ref=wave_hbm.at[:, f, pl.ds(0, HALO)], dst_ref=below_ref.at[f],
            send_sem=send_down.at[f], recv_sem=recv_down.at[f],
            device_id={fast: fast_me - 1}, device_id_type=MESH,
        )

    def mask_copy(i):
        return pltpu.make_async_remote_copy(
            src_ref=mask_ref.at[pl.ds(0 if i else receivers - HALO, HALO)], dst_ref=masks_ref.at[i],
            send_sem=send_mask.at[i], recv_sem=recv_mask.at[i],
            device_id={fast: fast_me - 1 if i else fast_me + 1}, device_id_type=MESH,
        )

    def edge_copy(i):
        return pltpu.make_async_remote_copy(
            src_ref=edge_ref, dst_ref=next_ref if i else prev_ref,
            send_sem=send_edge.at[i], recv_sem=recv_edge.at[i],
            device_id={slow: slow_me - 1 if i else slow_me + 1}, device_id_type=MESH,
        )

    def corner_copy(i, peer, rows):
        return pltpu.make_async_remote_copy(
            src_ref=edge_ref.at[rows], dst_ref=corner_ref.at[i],
            send_sem=send_corner.at[i], recv_sem=recv_corner.at[i],
            device_id=peer, device_id_type=MESH,
        )

    def send_halos(f):
        @pl.when(has_below)
        def _():
            up(f).start()

        @pl.when(has_above)
        def _():
            down(f).start()

    barrier = pltpu.get_barrier_semaphore()
    for d in range(1, slow_count):
        pl.semaphore_signal(barrier, inc=1, device_id=slow_peer(d), device_id_type=MESH)
    for d in range(1, fast_count):
        pl.semaphore_signal(barrier, inc=1, device_id=fast_peer(d), device_id_type=MESH)
    for i, there, came, peer, rows in corners:
        @pl.when(there)
        def _():
            pl.semaphore_signal(barrier, inc=1, device_id=peer, device_id_type=MESH)

    @pl.loop(0, slices)
    def _(f):
        load(f).start()

    band_copy = pltpu.make_async_copy(band_hbm, band_ref, band_sem)
    band_copy.start()

    zeros = jnp.zeros((STRIP, shots), jnp.bfloat16)
    for x in range(2):
        @pl.loop(0, high_ref.shape[1] // STRIP)
        def _(i):
            rows = pl.ds(pl.multiple_of(i * STRIP, STRIP), STRIP)
            high_ref[x, rows, :] = zeros
            low_ref[x, rows, :] = zeros

    @pl.when(jnp.logical_not(has_prev))
    def _():
        prev_ref[...] = jnp.zeros_like(prev_ref)

    @pl.when(jnp.logical_not(has_next))
    def _():
        next_ref[...] = jnp.zeros_like(next_ref)

    for i, there, came, peer, rows in corners:
        @pl.when(jnp.logical_not(came))
        def _():
            corner_ref[i] = jnp.zeros(corner_ref.shape[1:], jnp.float32)

    edge_ref[...] = jnp.zeros_like(edge_ref)
    greeted = sum(there.astype(jnp.int32) for _, there, *_ in corners)
    pl.semaphore_wait(barrier, slow_count + fast_count - 2 + greeted)

    @pl.when(has_below)
    def _():
        mask_copy(0).start()

    @pl.when(has_above)
    def _():
        mask_copy(1).start()

    for f in range(FIRST):
        send_halos(f)

    lane = lax.broadcasted_iota(jnp.int32, (BLOCK, LANES), 1)

    @pl.loop(0, slices)
    def _(f):
        load(f).wait()
        for b in range(blocks):
            rows = pl.ds(b * BLOCK, BLOCK)
            edges = edge_ref[rows, :]
            for x in range(2):
                place = 4 * f + 2 * x
                ours = (lane >= place) & (lane < place + 2)
                edges = jnp.where(ours, pltpu.roll(wave_ref[x, f, rows, :LANES], place, 1), edges)
                place = place + LANES // 2
                ours = (lane >= place) & (lane < place + 2)
                turned = pltpu.roll(wave_ref[x, f, rows, shots - LANES :], lax.rem(place + 2, LANES), 1)
                edges = jnp.where(ours, turned, edges)
            edge_ref[rows, :] = edges

    @pl.when(has_next)
    def _():
        edge_copy(0).start()

    @pl.when(has_prev)
    def _():
        edge_copy(1).start()

    for i, there, came, peer, rows in corners:
        @pl.when(there)
        def _():
            corner_copy(i, peer, rows).start()

    @pl.loop(FIRST, slices)
    def _(f):
        send_halos(f)

    source = lax.broadcasted_iota(jnp.int32, (2 * LANES, LANES), 0)
    source = jnp.where(source < LANES, source, jnp.where(source < LANES + LANES // 2, source, source - 2 * LANES))
    offset = source - lax.broadcasted_iota(jnp.int32, (2 * LANES, LANES), 1) + SHALF
    turn = jnp.zeros((2 * LANES, LANES), jnp.float32)
    for u in range(2 * SHALF + 1):
        turn = jnp.where(offset == u, taper_ref[u], turn)
    turn = jnp.concatenate(split(turn), axis=1)
    for i in range(2):
        turn_ref[2 * i * LANES : 2 * (i + 1) * LANES, :] = turn

    column = lax.broadcasted_iota(jnp.int32, (BLOCK, LANES), 1)

    def prepare(f):
        odd, slot = lax.rem(f, 2), lax.rem(f, 2)
        live = (column // APER) == odd
        lanes = pl.ds(pl.multiple_of(f // 2 * LANES, LANES), LANES)
        for block in range(blocks):
            for x in range(2):
                cells = jnp.where(live, band_ref[x, block * BLOCK : (block + 1) * BLOCK, lanes], 0.0)
                cells = pltpu.roll(cells, shift_ref[block] + SHIFT + APER * odd, 1)
                for h in range(2):
                    taps = pltpu.roll(cells[h * HALF : (h + 1) * HALF], 0, 1, stride=1, stride_axis=0)
                    weight_ref[slot, 2 * block + h, 0, x], weight_ref[slot, 2 * block + h, 1, x] = split(taps)

    band_copy.wait()
    prepare(0)

    @pl.when(has_above)
    def _():
        mask_copy(0).wait_recv()

    @pl.when(has_below)
    def _():
        mask_copy(1).wait_recv()

    @pl.when(has_prev)
    def _():
        edge_copy(0).wait_recv()

    @pl.when(has_next)
    def _():
        edge_copy(1).wait_recv()

    for i, there, came, peer, rows in corners:
        @pl.when(came)
        def _():
            corner_copy(i, peer, rows).wait_recv()

    def stage(x, f, wave, mask, after, before, at):
        count = wave.shape[0]
        tile = lax.broadcasted_iota(jnp.int32, (count, LANES), 1) < LANES // 2
        place = 4 * f + 2 * x
        after = pltpu.roll(after, lax.rem(LANES - place, LANES), 1)
        before = pltpu.roll(before, lax.rem(LANES + LANES // 2 - place - 2, LANES), 1)
        outside = split(jnp.where(tile, after, before) * mask)
        inside = [split(wave[:, i * LANES : (i + 1) * LANES] * mask) for i in range(shots // LANES)]
        cells = [outside, *inside, outside]
        parts = []
        for part in range(2):
            rows = []
            for i in range(shots // LANES):
                around = jnp.where(tile, cells[i + 2][part], cells[i][part])
                rows.append(jnp.concatenate([cells[i + 1][part], around], axis=1))
            parts.append(jnp.concatenate(rows, axis=0))
        both = jnp.dot(jnp.concatenate(parts, axis=1), turn_ref[...], preferred_element_type=jnp.float32)
        high, low = split(both[:, :LANES] + both[:, LANES:])
        rows = pl.ds(at, count)
        for i in range(shots // LANES):
            lanes = pl.ds(i * LANES, LANES)
            high_ref[x, rows, lanes] = high[i * count : (i + 1) * count]
            low_ref[x, rows, lanes] = low[i * count : (i + 1) * count]

    def predict(f, block):
        slot = lax.rem(f, 2)
        total = jnp.zeros((8, shots), jnp.float32)
        for h in range(2):
            half = 2 * block + h
            base = half * HALF
            parts = []
            for part in range(2):
                real, imag = weight_ref[slot, half, part, 0], weight_ref[slot, half, part, 1]
                parts.append(jnp.concatenate([real, -imag], axis=1))
                parts.append(jnp.concatenate([imag, real], axis=1))
            window = pl.ds(base, DEPTH)
            high = jnp.concatenate([high_ref[x, window, :] for x in range(2)], axis=0)
            low = jnp.concatenate([low_ref[x, window, :] for x in range(2)], axis=0)
            upper = jnp.dot(jnp.concatenate(parts, axis=0), high, preferred_element_type=jnp.float32)
            lower = jnp.dot(jnp.concatenate(parts[:2], axis=0), low, preferred_element_type=jnp.float32)
            pred = upper[:BLOCK] + (upper[BLOCK:] + lower)
            for x in range(2):
                mult_ref[x, f, pl.ds(base, HALF), :] = pred[x * HALF : (x + 1) * HALF]
            total = total + jnp.sum((pred * pred).reshape(-1, 8, shots), axis=0)
        return total

    def lanes_of(total):
        return sum(total[:, i * LANES : (i + 1) * LANES] for i in range(shots // LANES))

    @pl.loop(0, slices)
    def _(f):
        def own(i, data):
            rows = pl.ds(pl.multiple_of(i * BLOCK, BLOCK), BLOCK)
            at = pl.multiple_of(i * BLOCK + HALO, STRIP)
            for x in range(2):
                wave = wave_ref[x, f, rows, :]
                stage(x, f, wave, mask_ref[rows, :], next_ref[rows, :], prev_ref[rows, :], at)
                data = data + lanes_of(jnp.sum((wave * wave).reshape(-1, 8, shots), axis=0))
            return data

        data_ref[f] = lax.fori_loop(0, blocks, own, jnp.zeros((8, LANES), jnp.float32), unroll=True)

        prepare(jnp.minimum(f + 1, slices - 1))
        total = jnp.zeros((8, shots), jnp.float32)
        for block in range(1, blocks - 1):
            total = total + predict(f, block)

        @pl.when(has_above)
        def _():
            up(f).wait_recv()
            for x in range(2):
                stage(x, f, above_ref[f, x], masks_ref[0], corner_ref[1], corner_ref[0], 0)

        @pl.when(has_below)
        def _():
            down(f).wait_recv()
            for x in range(2):
                stage(x, f, below_ref[f, x], masks_ref[1], corner_ref[3], corner_ref[2], HALO + receivers)

        for block in sorted({0, blocks - 1}):
            total = total + predict(f, block)
        pred_ref[f] = lanes_of(total)

    row = lax.broadcasted_iota(jnp.int32, (8, LANES), 0)
    col = lax.broadcasted_iota(jnp.int32, (8, LANES), 1)
    mine = jnp.zeros((8, LANES), jnp.float32)
    for f in range(slices):
        mine = jnp.where((row == 0) & (col == f), jnp.sum(data_ref[f]), mine)
        mine = jnp.where((row == 1) & (col == f), jnp.sum(pred_ref[f]), mine)
    mine_ref[...] = mine

    own = pltpu.make_async_copy(mine_ref, plane_ref.at[0], own_sem)
    own.start()
    copies = []
    for d in range(1, slow_count):
        copy = pltpu.make_async_remote_copy(
            src_ref=mine_ref, dst_ref=plane_ref.at[d], send_sem=send_a.at[d], recv_sem=recv_a.at[d],
            device_id=slow_peer(d), device_id_type=MESH,
        )
        copy.start()
        copies.append(copy)
    own.wait()
    for copy in copies:
        copy.wait()
    copies = []
    for d in range(1, fast_count):
        copy = pltpu.make_async_remote_copy(
            src_ref=plane_ref, dst_ref=space_ref.at[d - 1], send_sem=send_b.at[d], recv_sem=recv_b.at[d],
            device_id=fast_peer(d), device_id_type=MESH,
        )
        copy.start()
        copies.append(copy)
    total = jnp.sum(plane_ref[...], axis=0)
    for copy in copies:
        copy.wait()
    for d in range(fast_count - 1):
        total = total + jnp.sum(space_ref[d], axis=0)
    data = jnp.broadcast_to(total[0:1], total.shape)
    pred = jnp.broadcast_to(total[1:2], total.shape)
    gain_ref[...] = jnp.sqrt((data + 1e-06) / (pred + 1e-06))

    @pl.when(has_below)
    def _():
        mask_copy(0).wait_send()

        @pl.loop(0, slices)
        def _(f):
            up(f).wait_send()

    @pl.when(has_above)
    def _():
        mask_copy(1).wait_send()

        @pl.loop(0, slices)
        def _(f):
            down(f).wait_send()

    @pl.when(has_next)
    def _():
        edge_copy(0).wait_send()

    @pl.when(has_prev)
    def _():
        edge_copy(1).wait_send()

    for i, there, came, peer, rows in corners:
        @pl.when(there)
        def _():
            corner_copy(i, peer, rows).wait_send()


def forward(axes, wave, band, shift, mask, taper):
    _, slices, receivers, shots = wave.shape
    slow_count, fast_count = axes[0][1], axes[1][1]
    tall = receivers + DEPTH - HALF
    dma = pltpu.SemaphoreType.DMA
    whole = pl.BlockSpec(memory_space=pltpu.VMEM)
    scalars = pl.BlockSpec(memory_space=pltpu.SMEM)
    hbm = pl.BlockSpec(memory_space=pltpu.HBM)
    return pl.pallas_call(
        functools.partial(forward_kernel, axes),
        in_specs=[scalars, scalars, whole, hbm, hbm],
        out_specs=[whole, whole, whole],
        out_shape=[
            jax.ShapeDtypeStruct(wave.shape, jnp.float32),
            jax.ShapeDtypeStruct(wave.shape, jnp.float32),
            jax.ShapeDtypeStruct((8, LANES), jnp.float32),
        ],
        scratch_shapes=[
            pltpu.VMEM(band.shape, jnp.float32),
            pltpu.VMEM((2, receivers // HALF, 2, 2, HALF, DEPTH), jnp.bfloat16),
            pltpu.VMEM((4 * LANES, 2 * LANES), jnp.bfloat16),
            pltpu.VMEM((2, tall, shots), jnp.bfloat16),
            pltpu.VMEM((2, tall, shots), jnp.bfloat16),
            pltpu.VMEM((slices, 2, HALO, shots), jnp.float32),
            pltpu.VMEM((slices, 2, HALO, shots), jnp.float32),
            pltpu.VMEM((receivers, LANES), jnp.float32),
            pltpu.VMEM((receivers, LANES), jnp.float32),
            pltpu.VMEM((receivers, LANES), jnp.float32),
            pltpu.VMEM((4, HALO, LANES), jnp.float32),
            pltpu.VMEM((2, HALO, LANES), jnp.float32),
            pltpu.VMEM((slices, 8, LANES), jnp.float32),
            pltpu.VMEM((slices, 8, LANES), jnp.float32),
            pltpu.VMEM((8, LANES), jnp.float32),
            pltpu.VMEM((slow_count, 8, LANES), jnp.float32),
            pltpu.VMEM((fast_count - 1, slow_count, 8, LANES), jnp.float32),
            dma((slices,)), dma, dma((slices,)), dma((slices,)), dma((slices,)), dma((slices,)),
            dma((2,)), dma((2,)), dma((2,)), dma((2,)), dma((4,)), dma((4,)), dma,
            dma((slow_count,)), dma((slow_count,)), dma((fast_count,)), dma((fast_count,)),
        ],
        cost_estimate=pl.CostEstimate(flops=2**33, bytes_accessed=wave.size * 8, transcendentals=0),
        compiler_params=pltpu.CompilerParams(
            collective_id=1, has_side_effects=True, vmem_limit_bytes=12 * 2**20
        ),
        name="forward",
    )(shift, taper, mask, wave, band)


def finish_kernel(gain_ref, wave_ref, mult_ref, mult_hbm, prim_hbm, prim_ref, mult_sem, prim_sem):
    slices = wave_ref.shape[1]
    slots = prim_ref.shape[0]

    def mult_copy(f):
        return pltpu.make_async_copy(mult_ref.at[:, f], mult_hbm.at[:, f], mult_sem.at[f])

    def prim_copy(f):
        return pltpu.make_async_copy(prim_ref.at[lax.rem(f, slots)], prim_hbm.at[:, f], prim_sem.at[f])

    col = lax.broadcasted_iota(jnp.int32, (1, LANES), 1)

    @pl.loop(0, slices)
    def _(f):
        mult_copy(f).start()
        gain = jnp.sum(jnp.where(col == f, gain_ref[0:1, :], 0.0))

        @pl.when(f >= slots)
        def _():
            prim_copy(f - slots).wait()

        for x in range(2):
            for r in range(0, wave_ref.shape[2], BLOCK):
                rows = pl.ds(r, BLOCK)
                prim_ref[lax.rem(f, slots), x, rows, :] = wave_ref[x, f, rows, :] - gain * mult_ref[x, f, rows, :]
        prim_copy(f).start()

    @pl.loop(0, slices)
    def _(f):
        mult_copy(f).wait()

    @pl.loop(max(slices - slots, 0), slices)
    def _(f):
        prim_copy(f).wait()


def finish(gain, wave, mult):
    slices = wave.shape[1]
    whole = pl.BlockSpec(memory_space=pltpu.VMEM)
    hbm = pl.BlockSpec(memory_space=pl.ANY)
    return pl.pallas_call(
        finish_kernel,
        in_specs=[whole, whole, whole],
        out_specs=[hbm, hbm],
        out_shape=[jax.ShapeDtypeStruct(wave.shape, jnp.float32)] * 2,
        scratch_shapes=[
            pltpu.VMEM((min(SLOTS, slices), 2, *wave.shape[2:]), jnp.float32),
            pltpu.SemaphoreType.DMA((slices,)),
            pltpu.SemaphoreType.DMA((slices,)),
        ],
        cost_estimate=pl.CostEstimate(flops=wave.size * 2, bytes_accessed=wave.size * 8, transcendentals=0),
        compiler_params=pltpu.CompilerParams(vmem_limit_bytes=12 * 2**20),
        name="finish",
    )(gain, wave, mult)


def per_device(wavefield, surface_band, band_shift, trace_mask, shot_taper):
    receivers = wavefield.shape[2]
    axes = (("src", lax.axis_size("src")), ("rcv", lax.axis_size("rcv")))
    mask = jnp.broadcast_to(trace_mask.astype(jnp.float32)[:, None], (receivers, LANES))
    wave, mult, gain = forward(axes, wavefield, surface_band, band_shift, mask, shot_taper)
    return tuple(finish(gain, wave, mult))


def solution(mesh):
    in_specs = (P(None, None, "rcv", "src"), P(None, "rcv", None), P("rcv"), P("rcv"), P())
    out_specs = (P(None, None, "rcv", "src"), P(None, None, "rcv", "src"))
    return jax.shard_map(
        per_device, mesh=mesh, in_specs=in_specs, out_specs=out_specs, check_vma=False
    )
```

```python
import functools

import jax
import jax.numpy as jnp
from jax import lax
from jax.experimental import pallas as pl
from jax.experimental.pallas import tpu as pltpu
from jax.sharding import PartitionSpec as P

APER = 64
SHIFT = 16
BLOCK = 64
HALF = BLOCK // 2
SHALF = 2
LANES = 128
DEPTH = 128
HALO = APER // 2 + SHIFT
FIRST = 3
GROUPS = 2
STRIP = 16
SLOTS = 8
MESH = pl.DeviceIdType.MESH


def split(cells):
    high = cells.astype(jnp.bfloat16)
    low = (cells - high.astype(jnp.float32)).astype(jnp.bfloat16)
    return high, low


def forward_kernel(axes, shift_hbm, taper_hbm, live_hbm, wave_hbm, band_hbm, *refs):
    wave_ref, mult_ref, gain_ref = refs[:3]
    (
        shift_ref, taper_ref, live_ref, mask_ref, band_ref, turn_ref,
        even_weight, odd_weight, even_high, odd_high, even_low, odd_low, above_ref, below_ref, edge_ref, next_ref, prev_ref, ends_ref, corner_ref, masks_ref,
        data_ref, inner_ref, outer_ref, mine_ref, plane_ref, space_ref,
        load_sem, small_sem, send_up, recv_up, send_down, recv_down, send_mask, recv_mask,
        send_edge, recv_edge, send_corner, recv_corner, send_a, recv_a, send_b, recv_b,
    ) = refs[3:]
    (slow, slow_count), (fast, fast_count) = axes
    slow_me, fast_me = lax.axis_index(slow), lax.axis_index(fast)
    _, slices, receivers, shots = wave_ref.shape
    blocks, group = receivers // BLOCK, slices // GROUPS
    share = 4 * group
    quarters = LANES // share
    has_above, has_below = fast_me > 0, fast_me < fast_count - 1
    has_prev, has_next = slow_me > 0, slow_me < slow_count - 1
    direct = slow_count * fast_count <= 32

    def peer_of(a, b):
        return {slow: lax.rem(slow_me + a, slow_count), fast: lax.rem(fast_me + b, fast_count)}

    corners = []
    for i, (down, right) in enumerate([(1, 1), (1, -1), (-1, 1), (-1, -1)]):
        there = (has_below if down > 0 else has_above) & (has_next if right > 0 else has_prev)
        came = (has_above if down > 0 else has_below) & (has_prev if right > 0 else has_next)
        corners.append((i, there, came, {fast: fast_me + down, slow: slow_me + right}, 0 if down > 0 else 1))

    def load(f):
        return pltpu.make_async_copy(wave_hbm.at[:, f], wave_ref.at[:, f], load_sem.at[f])

    def up(f):
        return pltpu.make_async_remote_copy(
            src_ref=wave_hbm.at[:, f, pl.ds(receivers - HALO, HALO)], dst_ref=above_ref.at[f],
            send_sem=send_up.at[f], recv_sem=recv_up.at[f],
            device_id={fast: fast_me + 1}, device_id_type=MESH,
        )

    def down(f):
        return pltpu.make_async_remote_copy(
            src_ref=wave_hbm.at[:, f, pl.ds(0, HALO)], dst_ref=below_ref.at[f],
            send_sem=send_down.at[f], recv_sem=recv_down.at[f],
            device_id={fast: fast_me - 1}, device_id_type=MESH,
        )

    def mask_copy(i):
        return pltpu.make_async_remote_copy(
            src_ref=mask_ref.at[pl.ds(0 if i else receivers - HALO, HALO)], dst_ref=masks_ref.at[i],
            send_sem=send_mask.at[i], recv_sem=recv_mask.at[i],
            device_id={fast: fast_me - 1 if i else fast_me + 1}, device_id_type=MESH,
        )

    def edge_copy(g, i):
        return pltpu.make_async_remote_copy(
            src_ref=edge_ref.at[g, 1 - i], dst_ref=next_ref.at[g] if i else prev_ref.at[g],
            send_sem=send_edge.at[g, i], recv_sem=recv_edge.at[g, i],
            device_id={slow: slow_me - 1 if i else slow_me + 1}, device_id_type=MESH,
        )

    def corner_copy(i, peer, end):
        return pltpu.make_async_remote_copy(
            src_ref=ends_ref.at[end], dst_ref=corner_ref.at[i],
            send_sem=send_corner.at[i], recv_sem=recv_corner.at[i],
            device_id=peer, device_id_type=MESH,
        )

    def send_halos(f):
        @pl.when(has_below)
        def _():
            up(f).start()

        @pl.when(has_above)
        def _():
            down(f).start()

    small = [
        pltpu.make_async_copy(a, b, small_sem.at[i])
        for i, (a, b) in enumerate(
            [(live_hbm, live_ref), (taper_hbm, taper_ref), (shift_hbm, shift_ref), (band_hbm, band_ref)]
        )
    ]
    for copy in small[:3]:
        copy.start()
    barrier = pltpu.get_barrier_semaphore()
    if direct:
        greeted = slow_count * fast_count - 1
        for a in range(slow_count):
            for b in range(fast_count):
                if a or b:
                    pl.semaphore_signal(barrier, inc=1, device_id=peer_of(a, b), device_id_type=MESH)
    else:
        greeted = slow_count + fast_count - 2 + sum(there.astype(jnp.int32) for _, there, *_ in corners)
        for a in range(1, slow_count):
            pl.semaphore_signal(barrier, inc=1, device_id=peer_of(a, 0), device_id_type=MESH)
        for b in range(1, fast_count):
            pl.semaphore_signal(barrier, inc=1, device_id=peer_of(0, b), device_id_type=MESH)
        for i, there, came, peer, end in corners:
            @pl.when(there)
            def _():
                pl.semaphore_signal(barrier, inc=1, device_id=peer, device_id_type=MESH)

    small[3].start()

    @pl.loop(0, slices)
    def _(f):
        load(f).start()

    small[0].wait()
    line = lax.broadcasted_iota(jnp.int32, (8, LANES), 0)

    @pl.loop(0, receivers // 8)
    def _(i):
        cells = jnp.zeros((8, LANES), jnp.float32)
        for r in range(8):
            cells = jnp.where(line == r, live_ref[i * 8 + r].astype(jnp.float32), cells)
        mask_ref[pl.ds(pl.multiple_of(i * 8, 8), 8), :] = cells

    small[1].wait()
    small[2].wait()

    source = lax.broadcasted_iota(jnp.int32, (2 * LANES, LANES), 0)
    source = jnp.where(source < LANES, source, jnp.where(source < LANES + LANES // 2, source, source - 2 * LANES))
    offset = source - lax.broadcasted_iota(jnp.int32, (2 * LANES, LANES), 1) + SHALF
    turn = jnp.zeros((2 * LANES, LANES), jnp.float32)
    for u in range(2 * SHALF + 1):
        turn = jnp.where(offset == u, taper_ref[u], turn)
    turn = jnp.concatenate(split(turn), axis=1)
    for i in range(2):
        turn_ref[2 * i * LANES : 2 * (i + 1) * LANES, :] = turn

    rows_refs, weight_refs = ((even_high, even_low), (odd_high, odd_low)), (even_weight, odd_weight)
    zeros = jnp.zeros((STRIP, shots), jnp.bfloat16)
    for x in range(2):
        @pl.loop(0, even_high.shape[1] // STRIP)
        def _(i):
            rows = pl.ds(pl.multiple_of(i * STRIP, STRIP), STRIP)
            for ref in (even_high, odd_high, even_low, odd_low):
                ref[x, rows, :] = zeros

    for there, ref in ((has_prev, prev_ref), (has_next, next_ref)):
        @pl.when(jnp.logical_not(there))
        def _():
            ref[...] = jnp.zeros_like(ref)

    for i, there, came, peer, end in corners:
        @pl.when(jnp.logical_not(came))
        def _():
            corner_ref[i] = jnp.zeros(corner_ref.shape[1:], jnp.float32)

    for i, (there, ref) in enumerate(((has_above, above_ref), (has_below, below_ref))):
        @pl.when(jnp.logical_not(there))
        def _():
            masks_ref[i] = jnp.zeros(masks_ref.shape[1:], jnp.float32)
            ref[0] = jnp.zeros(ref.shape[1:], jnp.float32)

    edge_ref[...] = jnp.zeros_like(edge_ref)

    column = lax.broadcasted_iota(jnp.int32, (BLOCK, LANES), 1)

    def prepare(f, odd):
        weight_ref = weight_refs[odd]
        live = (column // APER) == odd
        lanes = pl.ds(pl.multiple_of(f // 2 * LANES, LANES), LANES)
        for block in range(blocks):
            for x in range(2):
                cells = jnp.where(live, band_ref[x, block * BLOCK : (block + 1) * BLOCK, lanes], 0.0)
                cells = pltpu.roll(cells, shift_ref[block] + SHIFT + APER * odd, 1)
                for h in range(2):
                    taps = pltpu.roll(cells[h * HALF : (h + 1) * HALF], 0, 1, stride=1, stride_axis=0)
                    weight_ref[2 * block + h, 0, x], weight_ref[2 * block + h, 1, x] = split(taps)

    small[3].wait()
    prepare(0, 0)
    prepare(1, 1)

    pl.semaphore_wait(barrier, greeted)

    for f in range(FIRST):
        send_halos(f)

    @pl.when(has_below)
    def _():
        mask_copy(0).start()

    @pl.when(has_above)
    def _():
        mask_copy(1).start()

    lane = lax.broadcasted_iota(jnp.int32, (BLOCK, LANES), 1)

    def packed(block):
        return pl.ds(block // quarters * BLOCK, BLOCK), block % quarters * share

    for g in range(GROUPS):
        @pl.loop(0, group)
        def _(i):
            f = g * group + i
            load(f).wait()
            for chunk in range(0, blocks, quarters):
                rows, _ = packed(chunk)
                first, last = edge_ref[g, 0, rows, :], edge_ref[g, 1, rows, :]
                for block in range(chunk, min(chunk + quarters, blocks)):
                    cells = pl.ds(block * BLOCK, BLOCK)
                    for x in range(2):
                        place = packed(block)[1] + 4 * i + 2 * x
                        ours = (lane >= place) & (lane < place + 2)
                        first = jnp.where(ours, pltpu.roll(wave_ref[x, f, cells, :LANES], place, 1), first)
                        turned = pltpu.roll(wave_ref[x, f, cells, shots - LANES :], lax.rem(place + 2, LANES), 1)
                        last = jnp.where(ours, turned, last)
                edge_ref[g, 0, rows, :] = first
                edge_ref[g, 1, rows, :] = last

        @pl.when(has_next)
        def _():
            edge_copy(g, 0).start()

        @pl.when(has_prev)
        def _():
            edge_copy(g, 1).start()

    wide = lax.broadcasted_iota(jnp.int32, (HALO, LANES), 1)
    for end, block, skip in ((0, blocks - 1, BLOCK - HALO), (1, 0, 0)):
        cells = jnp.zeros((HALO, LANES), jnp.float32)
        rows, place = packed(block)
        for side in range(2):
            for g in range(GROUPS):
                spot = side * LANES // 2 + g * share
                part = pltpu.roll(edge_ref[g, side, rows, :][skip : skip + HALO], (spot - place) % LANES, 1)
                cells = jnp.where((wide >= spot) & (wide < spot + share), part, cells)
        ends_ref[end] = cells

    for i, there, came, peer, end in corners:
        @pl.when(there)
        def _():
            corner_copy(i, peer, end).start()

    @pl.loop(FIRST, slices)
    def _(f):
        send_halos(f)

    def turned(after, before, at_after, at_before):
        count = after.shape[0]
        after = pltpu.roll(after, lax.rem(LANES - at_after, LANES), 1)
        before = pltpu.roll(before, lax.rem(2 * LANES - 2 - at_before, LANES), 1)
        return jnp.where(lax.broadcasted_iota(jnp.int32, (count, LANES), 1) < LANES // 2, after, before)

    def stage(odd, x, wave, mask, outside, at):
        high_ref, low_ref = rows_refs[odd]
        count = wave.shape[0]
        tile = lax.broadcasted_iota(jnp.int32, (count, LANES), 1) < LANES // 2
        outside = split(outside * mask)
        inside = [split(wave[:, i * LANES : (i + 1) * LANES] * mask) for i in range(shots // LANES)]
        cells = [outside, *inside, outside]
        parts = []
        for part in range(2):
            rows = []
            for i in range(shots // LANES):
                around = jnp.where(tile, cells[i + 2][part], cells[i][part])
                rows.append(jnp.concatenate([cells[i + 1][part], around], axis=1))
            parts.append(jnp.concatenate(rows, axis=0))
        both = jnp.dot(jnp.concatenate(parts, axis=1), turn_ref[...], preferred_element_type=jnp.float32)
        high, low = split(both[:, :LANES] + both[:, LANES:])
        rows = pl.ds(at, count)
        for i in range(shots // LANES):
            lanes = pl.ds(i * LANES, LANES)
            high_ref[x, rows, lanes] = high[i * count : (i + 1) * count]
            low_ref[x, rows, lanes] = low[i * count : (i + 1) * count]

    def predict(f, odd, block):
        (high_ref, low_ref), weight_ref = rows_refs[odd], weight_refs[odd]
        total = jnp.zeros((8, shots), jnp.float32)
        for h in range(2):
            half = 2 * block + h
            base = half * HALF
            parts = []
            for part in range(2):
                real, imag = weight_ref[half, part, 0], weight_ref[half, part, 1]
                parts.append(jnp.concatenate([real, -imag], axis=1))
                parts.append(jnp.concatenate([imag, real], axis=1))
            window = pl.ds(base, DEPTH)
            high = jnp.concatenate([high_ref[x, window, :] for x in range(2)], axis=0)
            low = jnp.concatenate([low_ref[x, window, :] for x in range(2)], axis=0)
            upper = jnp.dot(jnp.concatenate(parts, axis=0), high, preferred_element_type=jnp.float32)
            lower = jnp.dot(jnp.concatenate(parts[:2], axis=0), low, preferred_element_type=jnp.float32)
            pred = upper[:BLOCK] + (upper[BLOCK:] + lower)
            for x in range(2):
                mult_ref[x, f, pl.ds(base, HALF), :] = pred[x * HALF : (x + 1) * HALF]
            total = total + jnp.sum((pred * pred).reshape(-1, 8, shots), axis=0)
        return total

    def lanes_of(total):
        return sum(total[:, i * LANES : (i + 1) * LANES] for i in range(shots // LANES))

    def wait_edges(g):
        @pl.when(has_prev)
        def _():
            edge_copy(g, 0).wait_recv()

        @pl.when(has_next)
        def _():
            edge_copy(g, 1).wait_recv()

    def wait_halos(f):
        @pl.when(has_above)
        def _():
            up(f).wait_recv()

        @pl.when(has_below)
        def _():
            down(f).wait_recv()

    def stage_own(f, odd):
        g, i = f // group, lax.rem(f, group)
        data = jnp.zeros((8, LANES), jnp.float32)
        for block in range(blocks):
            rows = pl.ds(block * BLOCK, BLOCK)
            cells, place = packed(block)
            after, before = next_ref[g, cells, :], prev_ref[g, cells, :]
            for x in range(2):
                wave = wave_ref[x, f, rows, :]
                at = place + 4 * i + 2 * x
                stage(odd, x, wave, mask_ref[rows, :], turned(after, before, at, at), block * BLOCK + HALO)
                data = data + lanes_of(jnp.sum((wave * wave).reshape(-1, 8, shots), axis=0))
        data_ref[f] = data

    def stage_halos(f, odd):
        for x in range(2):
            at = 4 * f + 2 * x
            for k, (ref, start, there) in enumerate(
                ((above_ref, 0, has_above), (below_ref, HALO + receivers, has_below))
            ):
                outside = turned(corner_ref[2 * k + 1], corner_ref[2 * k], at, LANES // 2 + at)
                stage(odd, x, ref[f * there.astype(jnp.int32), x], masks_ref[k], outside, start)

    def predict_inner(f, odd):
        total = jnp.zeros((8, shots), jnp.float32)
        for block in range(1, blocks - 1):
            total = total + predict(f, odd, block)
        inner_ref[f] = lanes_of(total)

    def predict_outer(f, odd):
        total = jnp.zeros((8, shots), jnp.float32)
        for block in sorted({0, blocks - 1}):
            total = total + predict(f, odd, block)
        outer_ref[f] = lanes_of(total)

    def step(f, odd):
        wait_halos(f)
        stage_halos(f, odd)
        stage_own(f + 1, 1 - odd)
        predict_outer(f, odd)
        predict_inner(f + 1, 1 - odd)

    wait_edges(0)
    stage_own(0, 0)
    predict_inner(0, 0)

    @pl.when(has_above)
    def _():
        mask_copy(0).wait_recv()

    @pl.when(has_below)
    def _():
        mask_copy(1).wait_recv()

    for i, there, came, peer, end in corners:
        @pl.when(came)
        def _():
            corner_copy(i, peer, end).wait_recv()

    @pl.loop(0, slices // 2 - 1)
    def _(pair):
        f = 2 * pair
        step(f, 0)
        prepare(f + 2, 0)
        for g in range(1, GROUPS):
            @pl.when(f + 2 == g * group)
            def _():
                wait_edges(g)

        step(f + 1, 1)
        prepare(f + 3, 1)

    step(slices - 2, 0)
    wait_halos(slices - 1)
    stage_halos(slices - 1, 1)
    predict_outer(slices - 1, 1)

    cells = jnp.concatenate([jnp.sum(data_ref[...], axis=1), jnp.sum(inner_ref[...] + outer_ref[...], axis=1)], axis=0)
    row = lax.broadcasted_iota(jnp.int32, cells.shape, 0)
    col = lax.broadcasted_iota(jnp.int32, cells.shape, 1)
    spot = jnp.where(row < slices, row, row - slices + LANES // 2)
    cells = jnp.where(col == spot, jnp.sum(cells, axis=1, keepdims=True), 0.0)
    mine = jnp.sum(cells, axis=0, keepdims=True)
    mine_ref[...] = mine

    def exchange(source, target, pairs, send, recv):
        copies = []
        for n, (a, b) in enumerate(pairs):
            copy = pltpu.make_async_remote_copy(
                src_ref=source, dst_ref=target.at[n], send_sem=send.at[n], recv_sem=recv.at[n],
                device_id=peer_of(a, b), device_id_type=MESH,
            )
            copy.start()
            copies.append(copy)
        for copy in copies:
            copy.wait()

    if direct:
        pairs = [(a, b) for b in range(fast_count) for a in range(slow_count) if a or b]
        exchange(mine_ref, space_ref, pairs, send_b, recv_b)
        total = mine + jnp.sum(space_ref[...], axis=0)
    else:
        exchange(mine_ref, plane_ref, [(a, 0) for a in range(1, slow_count)], send_a, recv_a)
        total = mine + jnp.sum(plane_ref[...], axis=0)
        mine_ref[...] = total
        exchange(mine_ref, space_ref, [(0, b) for b in range(1, fast_count)], send_b, recv_b)
        total = total + jnp.sum(space_ref[...], axis=0)
    gain_ref[...] = jnp.sqrt((total + 1e-06) / (pltpu.roll(total, LANES // 2, 1) + 1e-06))

    @pl.when(has_below)
    def _():
        mask_copy(0).wait_send()

        @pl.loop(0, slices)
        def _(f):
            up(f).wait_send()

    @pl.when(has_above)
    def _():
        mask_copy(1).wait_send()

        @pl.loop(0, slices)
        def _(f):
            down(f).wait_send()

    for g in range(GROUPS):
        @pl.when(has_next)
        def _():
            edge_copy(g, 0).wait_send()

        @pl.when(has_prev)
        def _():
            edge_copy(g, 1).wait_send()

    for i, there, came, peer, end in corners:
        @pl.when(there)
        def _():
            corner_copy(i, peer, end).wait_send()


def forward(axes, wave, band, shift, live, taper):
    _, slices, receivers, shots = wave.shape
    slow_count, fast_count = axes[0][1], axes[1][1]
    direct = slow_count * fast_count <= 32
    peers = slow_count * fast_count - 1 if direct else fast_count - 1
    tall = receivers + DEPTH - HALF
    blocks, quarters = receivers // BLOCK, LANES // (4 * slices // GROUPS)
    packed = -(-blocks // quarters) * BLOCK
    dma = pltpu.SemaphoreType.DMA
    whole = pl.BlockSpec(memory_space=pltpu.VMEM)
    hbm = pl.BlockSpec(memory_space=pltpu.HBM)
    return pl.pallas_call(
        functools.partial(forward_kernel, axes),
        in_specs=[hbm] * 5,
        out_specs=[whole, whole, whole],
        out_shape=[
            jax.ShapeDtypeStruct(wave.shape, jnp.float32),
            jax.ShapeDtypeStruct(wave.shape, jnp.float32),
            jax.ShapeDtypeStruct((1, LANES), jnp.float32),
        ],
        scratch_shapes=[
            pltpu.SMEM(shift.shape, jnp.int32),
            pltpu.SMEM(taper.shape, jnp.float32),
            pltpu.SMEM(live.shape, jnp.int32),
            pltpu.VMEM((receivers, LANES), jnp.float32),
            pltpu.VMEM(band.shape, jnp.float32),
            pltpu.VMEM((4 * LANES, 2 * LANES), jnp.bfloat16),
            *[pltpu.VMEM((receivers // HALF, 2, 2, HALF, DEPTH), jnp.bfloat16)] * 2,
            *[pltpu.VMEM((2, tall, shots), jnp.bfloat16)] * 4,
            pltpu.VMEM((slices, 2, HALO, shots), jnp.float32),
            pltpu.VMEM((slices, 2, HALO, shots), jnp.float32),
            pltpu.VMEM((GROUPS, 2, packed, LANES), jnp.float32),
            pltpu.VMEM((GROUPS, packed, LANES), jnp.float32),
            pltpu.VMEM((GROUPS, packed, LANES), jnp.float32),
            pltpu.VMEM((2, HALO, LANES), jnp.float32),
            pltpu.VMEM((4, HALO, LANES), jnp.float32),
            pltpu.VMEM((2, HALO, LANES), jnp.float32),
            *[pltpu.VMEM((slices, 8, LANES), jnp.float32)] * 3,
            pltpu.VMEM((1, LANES), jnp.float32),
            pltpu.VMEM((slow_count - 1, 1, LANES), jnp.float32),
            pltpu.VMEM((peers, 1, LANES), jnp.float32),
            dma((slices,)), dma((4,)), dma((slices,)), dma((slices,)), dma((slices,)), dma((slices,)),
            dma((2,)), dma((2,)), dma((GROUPS, 2)), dma((GROUPS, 2)), dma((4,)), dma((4,)),
            dma((slow_count - 1,)), dma((slow_count - 1,)), dma((peers,)), dma((peers,)),
        ],
        cost_estimate=pl.CostEstimate(flops=2**33, bytes_accessed=wave.size * 8, transcendentals=0),
        compiler_params=pltpu.CompilerParams(
            collective_id=1, has_side_effects=True, vmem_limit_bytes=14 * 2**20
        ),
        name="forward",
    )(shift, taper, live, wave, band)


def finish_kernel(gain_ref, wave_ref, mult_ref, mult_hbm, prim_hbm, prim_ref, mult_sem, prim_sem):
    slices = wave_ref.shape[1]
    slots = prim_ref.shape[0]

    def mult_copy(f):
        return pltpu.make_async_copy(mult_ref.at[:, f], mult_hbm.at[:, f], mult_sem.at[f])

    def prim_copy(f):
        return pltpu.make_async_copy(prim_ref.at[lax.rem(f, slots)], prim_hbm.at[:, f], prim_sem.at[f])

    col = lax.broadcasted_iota(jnp.int32, (1, LANES), 1)

    @pl.loop(0, slices)
    def _(f):
        mult_copy(f).start()
        gain = jnp.sum(jnp.where(col == f, gain_ref[...], 0.0))

        @pl.when(f >= slots)
        def _():
            prim_copy(f - slots).wait()

        for x in range(2):
            for r in range(0, wave_ref.shape[2], BLOCK):
                rows = pl.ds(r, BLOCK)
                prim_ref[lax.rem(f, slots), x, rows, :] = wave_ref[x, f, rows, :] - gain * mult_ref[x, f, rows, :]
        prim_copy(f).start()

    @pl.loop(0, slices)
    def _(f):
        mult_copy(f).wait()

    @pl.loop(max(slices - slots, 0), slices)
    def _(f):
        prim_copy(f).wait()


def finish(gain, wave, mult):
    slices = wave.shape[1]
    whole = pl.BlockSpec(memory_space=pltpu.VMEM)
    hbm = pl.BlockSpec(memory_space=pl.ANY)
    return pl.pallas_call(
        finish_kernel,
        in_specs=[whole, whole, whole],
        out_specs=[hbm, hbm],
        out_shape=[jax.ShapeDtypeStruct(wave.shape, jnp.float32)] * 2,
        scratch_shapes=[
            pltpu.VMEM((min(SLOTS, slices), 2, *wave.shape[2:]), jnp.float32),
            pltpu.SemaphoreType.DMA((slices,)),
            pltpu.SemaphoreType.DMA((slices,)),
        ],
        cost_estimate=pl.CostEstimate(flops=wave.size * 2, bytes_accessed=wave.size * 8, transcendentals=0),
        compiler_params=pltpu.CompilerParams(vmem_limit_bytes=12 * 2**20),
        name="finish",
    )(gain, wave, mult)


def per_device(wavefield, surface_band, band_shift, trace_mask, shot_taper):
    axes = (("src", lax.axis_size("src")), ("rcv", lax.axis_size("rcv")))
    def keep(array):
        return pltpu.with_memory_space_constraint(array, pltpu.HBM) if array.size > 1 else array

    small = [keep(array) for array in (surface_band, band_shift, trace_mask, shot_taper)]
    wave, mult, gain = forward(axes, wavefield, *small)
    return tuple(finish(gain, wave, mult))


def solution(mesh):
    in_specs = (P(None, None, "rcv", "src"), P(None, "rcv", None), P("rcv"), P("rcv"), P())
    out_specs = (P(None, None, "rcv", "src"), P(None, None, "rcv", "src"))
    return jax.shard_map(
        per_device, mesh=mesh, in_specs=in_specs, out_specs=out_specs, check_vma=False
    )
```

```python
import functools

import jax
import jax.numpy as jnp
from jax import lax
from jax.experimental import pallas as pl
from jax.experimental.pallas import tpu as pltpu
from jax.sharding import PartitionSpec as P

APER = 64
SHIFT = 16
BLOCK = 64
HALF = BLOCK // 2
SHALF = 2
LANES = 128
DEPTH = 128
HALO = APER // 2 + SHIFT
FIRST = 3
GROUPS = 2
STRIP = 16
SLOTS = 8
MESH = pl.DeviceIdType.MESH


def split(cells):
    high = cells.astype(jnp.bfloat16)
    low = (cells - high.astype(jnp.float32)).astype(jnp.bfloat16)
    return high, low


def forward_kernel(axes, shift_hbm, taper_hbm, live_hbm, wave_hbm, band_hbm, *refs):
    wave_ref, mult_ref, gain_ref = refs[:3]
    (
        shift_ref, taper_ref, live_ref, mask_ref, band_ref, turn_ref,
        even_weight, odd_weight, even_high, odd_high, even_low, odd_low, above_ref, below_ref, edge_ref, next_ref, prev_ref, ends_ref, corner_ref, masks_ref,
        data_ref, inner_ref, outer_ref, mine_ref, plane_ref, space_ref,
        load_sem, small_sem, send_up, recv_up, send_down, recv_down, send_mask, recv_mask,
        send_edge, recv_edge, send_corner, recv_corner, send_a, recv_a, send_b, recv_b, flood_sem,
    ) = refs[3:]
    (slow, slow_count), (fast, fast_count) = axes
    slow_me, fast_me = lax.axis_index(slow), lax.axis_index(fast)
    _, slices, receivers, shots = wave_ref.shape
    blocks, group = receivers // BLOCK, slices // GROUPS
    share = 4 * group
    quarters = LANES // share
    has_above, has_below = fast_me > 0, fast_me < fast_count - 1
    has_prev, has_next = slow_me > 0, slow_me < slow_count - 1
    direct = slow_count * fast_count <= 32

    def peer_of(a, b):
        return {slow: lax.rem(slow_me + a, slow_count), fast: lax.rem(fast_me + b, fast_count)}

    corners = []
    for i, (down, right) in enumerate([(1, 1), (1, -1), (-1, 1), (-1, -1)]):
        there = (has_below if down > 0 else has_above) & (has_next if right > 0 else has_prev)
        came = (has_above if down > 0 else has_below) & (has_prev if right > 0 else has_next)
        corners.append((i, there, came, {fast: fast_me + down, slow: slow_me + right}, 0 if down > 0 else 1))

    def load(f):
        return pltpu.make_async_copy(wave_hbm.at[:, f], wave_ref.at[:, f], load_sem.at[f])

    def up(f):
        return pltpu.make_async_remote_copy(
            src_ref=wave_hbm.at[:, f, pl.ds(receivers - HALO, HALO)], dst_ref=above_ref.at[f],
            send_sem=send_up.at[f], recv_sem=recv_up.at[f],
            device_id={fast: fast_me + 1}, device_id_type=MESH,
        )

    def down(f):
        return pltpu.make_async_remote_copy(
            src_ref=wave_hbm.at[:, f, pl.ds(0, HALO)], dst_ref=below_ref.at[f],
            send_sem=send_down.at[f], recv_sem=recv_down.at[f],
            device_id={fast: fast_me - 1}, device_id_type=MESH,
        )

    def mask_copy(i):
        return pltpu.make_async_remote_copy(
            src_ref=mask_ref.at[pl.ds(0 if i else receivers - HALO, HALO)], dst_ref=masks_ref.at[i],
            send_sem=send_mask.at[i], recv_sem=recv_mask.at[i],
            device_id={fast: fast_me - 1 if i else fast_me + 1}, device_id_type=MESH,
        )

    def edge_copy(g, i):
        return pltpu.make_async_remote_copy(
            src_ref=edge_ref.at[g, 1 - i], dst_ref=next_ref.at[g] if i else prev_ref.at[g],
            send_sem=send_edge.at[g, i], recv_sem=recv_edge.at[g, i],
            device_id={slow: slow_me - 1 if i else slow_me + 1}, device_id_type=MESH,
        )

    def corner_copy(i, peer, end):
        return pltpu.make_async_remote_copy(
            src_ref=ends_ref.at[end], dst_ref=corner_ref.at[i],
            send_sem=send_corner.at[i], recv_sem=recv_corner.at[i],
            device_id=peer, device_id_type=MESH,
        )

    def send_halos(f):
        @pl.when(has_below)
        def _():
            up(f).start()

        @pl.when(has_above)
        def _():
            down(f).start()

    small = [
        pltpu.make_async_copy(a, b, small_sem.at[i])
        for i, (a, b) in enumerate(
            [(live_hbm, live_ref), (taper_hbm, taper_ref), (shift_hbm, shift_ref), (band_hbm, band_ref)]
        )
    ]
    for copy in small[:3]:
        copy.start()
    barrier = pltpu.get_barrier_semaphore()
    near = [
        (has_above, {fast: fast_me - 1}), (has_below, {fast: fast_me + 1}),
        (has_prev, {slow: slow_me - 1}), (has_next, {slow: slow_me + 1}),
    ]
    beside = sum(there.astype(jnp.int32) for there, _ in near)
    greeted = beside + sum(there.astype(jnp.int32) for _, there, *_ in corners)
    for there, peer in near + [(there, peer) for _, there, _, peer, _ in corners]:
        @pl.when(there)
        def _():
            pl.semaphore_signal(barrier, inc=1, device_id=peer, device_id_type=MESH)

    small[3].start()

    @pl.loop(0, slices)
    def _(f):
        load(f).start()

    pl.semaphore_wait(barrier, greeted)

    for f in range(FIRST):
        send_halos(f)

    small[0].wait()
    line = lax.broadcasted_iota(jnp.int32, (8, LANES), 0)

    @pl.loop(0, receivers // 8, unroll=4)
    def _(i):
        cells = jnp.zeros((8, LANES), jnp.float32)
        for r in range(8):
            cells = jnp.where(line == r, live_ref[i * 8 + r].astype(jnp.float32), cells)
        mask_ref[pl.ds(pl.multiple_of(i * 8, 8), 8), :] = cells

    @pl.when(has_below)
    def _():
        mask_copy(0).start()

    @pl.when(has_above)
    def _():
        mask_copy(1).start()

    small[1].wait()
    small[2].wait()

    source = lax.broadcasted_iota(jnp.int32, (2 * LANES, LANES), 0)
    source = jnp.where(source < LANES, source, jnp.where(source < LANES + LANES // 2, source, source - 2 * LANES))
    offset = source - lax.broadcasted_iota(jnp.int32, (2 * LANES, LANES), 1) + SHALF
    turn = jnp.zeros((2 * LANES, LANES), jnp.float32)
    for u in range(2 * SHALF + 1):
        turn = jnp.where(offset == u, taper_ref[u], turn)
    turn = jnp.concatenate(split(turn), axis=1)
    for i in range(2):
        turn_ref[2 * i * LANES : 2 * (i + 1) * LANES, :] = turn

    rows_refs, weight_refs = ((even_high, even_low), (odd_high, odd_low)), (even_weight, odd_weight)
    for there, ref in ((has_prev, prev_ref), (has_next, next_ref)):
        @pl.when(jnp.logical_not(there))
        def _():
            ref[...] = jnp.zeros_like(ref)

    for i, there, came, peer, end in corners:
        @pl.when(jnp.logical_not(came))
        def _():
            corner_ref[i] = jnp.zeros(corner_ref.shape[1:], jnp.float32)

    for i, (there, ref) in enumerate(((has_above, above_ref), (has_below, below_ref))):
        @pl.when(jnp.logical_not(there))
        def _():
            masks_ref[i] = jnp.zeros(masks_ref.shape[1:], jnp.float32)
            ref[0] = jnp.zeros(ref.shape[1:], jnp.float32)

    edge_ref[...] = jnp.zeros_like(edge_ref)

    column = lax.broadcasted_iota(jnp.int32, (BLOCK, LANES), 1)

    def prepare(f, odd):
        weight_ref = weight_refs[odd]
        live = (column // APER) == odd
        lanes = pl.ds(pl.multiple_of(f // 2 * LANES, LANES), LANES)
        for block in range(blocks):
            for x in range(2):
                cells = jnp.where(live, band_ref[x, block * BLOCK : (block + 1) * BLOCK, lanes], 0.0)
                cells = pltpu.roll(cells, shift_ref[block] + SHIFT + APER * odd, 1)
                for h in range(2):
                    taps = pltpu.roll(cells[h * HALF : (h + 1) * HALF], 0, 1, stride=1, stride_axis=0)
                    weight_ref[2 * block + h, 0, x], weight_ref[2 * block + h, 1, x] = split(taps)

    small[3].wait()
    prepare(0, 0)

    lane = lax.broadcasted_iota(jnp.int32, (BLOCK, LANES), 1)

    def packed(block):
        return pl.ds(block // quarters * BLOCK, BLOCK), block % quarters * share

    for g in range(GROUPS):
        @pl.loop(0, group, unroll=2)
        def _(i):
            f = g * group + i
            load(f).wait()
            for chunk in range(0, blocks, quarters):
                rows, _ = packed(chunk)
                first, last = edge_ref[g, 0, rows, :], edge_ref[g, 1, rows, :]
                for block in range(chunk, min(chunk + quarters, blocks)):
                    cells = pl.ds(block * BLOCK, BLOCK)
                    for x in range(2):
                        place = packed(block)[1] + 4 * i + 2 * x
                        ours = (lane >= place) & (lane < place + 2)
                        first = jnp.where(ours, pltpu.roll(wave_ref[x, f, cells, :LANES], place, 1), first)
                        turned = pltpu.roll(wave_ref[x, f, cells, shots - LANES :], lax.rem(place + 2, LANES), 1)
                        last = jnp.where(ours, turned, last)
                edge_ref[g, 0, rows, :] = first
                edge_ref[g, 1, rows, :] = last

        @pl.when(has_next)
        def _():
            edge_copy(g, 0).start()

        @pl.when(has_prev)
        def _():
            edge_copy(g, 1).start()

    wide = lax.broadcasted_iota(jnp.int32, (HALO, LANES), 1)
    for end, block, skip in ((0, blocks - 1, BLOCK - HALO), (1, 0, 0)):
        cells = jnp.zeros((HALO, LANES), jnp.float32)
        rows, place = packed(block)
        for side in range(2):
            for g in range(GROUPS):
                spot = side * LANES // 2 + g * share
                part = pltpu.roll(edge_ref[g, side, rows, :][skip : skip + HALO], (spot - place) % LANES, 1)
                cells = jnp.where((wide >= spot) & (wide < spot + share), part, cells)
        ends_ref[end] = cells

    for i, there, came, peer, end in corners:
        @pl.when(there)
        def _():
            corner_copy(i, peer, end).start()

    @pl.loop(FIRST, slices)
    def _(f):
        send_halos(f)

    def turned(after, before, at_after, at_before):
        count = after.shape[0]
        after = pltpu.roll(after, lax.rem(LANES - at_after, LANES), 1)
        before = pltpu.roll(before, lax.rem(2 * LANES - 2 - at_before, LANES), 1)
        return jnp.where(lax.broadcasted_iota(jnp.int32, (count, LANES), 1) < LANES // 2, after, before)

    def stage(odd, x, wave, mask, outside, at):
        high_ref, low_ref = rows_refs[odd]
        count = wave.shape[0]
        tile = lax.broadcasted_iota(jnp.int32, (count, LANES), 1) < LANES // 2
        outside = split(outside * mask)
        inside = [split(wave[:, i * LANES : (i + 1) * LANES] * mask) for i in range(shots // LANES)]
        cells = [outside, *inside, outside]
        parts = []
        for part in range(2):
            rows = []
            for i in range(shots // LANES):
                around = jnp.where(tile, cells[i + 2][part], cells[i][part])
                rows.append(jnp.concatenate([cells[i + 1][part], around], axis=1))
            parts.append(jnp.concatenate(rows, axis=0))
        both = jnp.dot(jnp.concatenate(parts, axis=1), turn_ref[...], preferred_element_type=jnp.float32)
        high, low = split(both[:, :LANES] + both[:, LANES:])
        rows = pl.ds(at, count)
        for i in range(shots // LANES):
            lanes = pl.ds(i * LANES, LANES)
            high_ref[x, rows, lanes] = high[i * count : (i + 1) * count]
            low_ref[x, rows, lanes] = low[i * count : (i + 1) * count]

    def predict(f, odd, block):
        (high_ref, low_ref), weight_ref = rows_refs[odd], weight_refs[odd]
        total = jnp.zeros((8, shots), jnp.float32)
        for h in range(2):
            half = 2 * block + h
            base = half * HALF
            parts = []
            for part in range(2):
                real, imag = weight_ref[half, part, 0], weight_ref[half, part, 1]
                parts.append(jnp.concatenate([real, -imag], axis=1))
                parts.append(jnp.concatenate([imag, real], axis=1))
            window = pl.ds(base, DEPTH)
            high = jnp.concatenate([high_ref[x, window, :] for x in range(2)], axis=0)
            low = jnp.concatenate([low_ref[x, window, :] for x in range(2)], axis=0)
            upper = jnp.dot(jnp.concatenate(parts, axis=0), high, preferred_element_type=jnp.float32)
            lower = jnp.dot(jnp.concatenate(parts[:2], axis=0), low, preferred_element_type=jnp.float32)
            pred = upper[:BLOCK] + (upper[BLOCK:] + lower)
            for x in range(2):
                mult_ref[x, f, pl.ds(base, HALF), :] = pred[x * HALF : (x + 1) * HALF]
            total = total + jnp.sum((pred * pred).reshape(-1, 8, shots), axis=0)
        return total

    def lanes_of(total):
        return sum(total[:, i * LANES : (i + 1) * LANES] for i in range(shots // LANES))

    def wait_edges(g):
        @pl.when(has_prev)
        def _():
            edge_copy(g, 0).wait_recv()

        @pl.when(has_next)
        def _():
            edge_copy(g, 1).wait_recv()

    def wait_halos(f):
        @pl.when(has_above)
        def _():
            up(f).wait_recv()

        @pl.when(has_below)
        def _():
            down(f).wait_recv()

    def stage_own(f, odd):
        g, i = f // group, lax.rem(f, group)
        data = jnp.zeros((8, LANES), jnp.float32)
        for block in range(blocks):
            rows = pl.ds(block * BLOCK, BLOCK)
            cells, place = packed(block)
            after, before = next_ref[g, cells, :], prev_ref[g, cells, :]
            for x in range(2):
                wave = wave_ref[x, f, rows, :]
                at = place + 4 * i + 2 * x
                stage(odd, x, wave, mask_ref[rows, :], turned(after, before, at, at), block * BLOCK + HALO)
                data = data + lanes_of(jnp.sum((wave * wave).reshape(-1, 8, shots), axis=0))
        data_ref[f] = data

    def stage_halos(f, odd):
        for x in range(2):
            at = 4 * f + 2 * x
            for k, (ref, start, there) in enumerate(
                ((above_ref, 0, has_above), (below_ref, HALO + receivers, has_below))
            ):
                outside = turned(corner_ref[2 * k + 1], corner_ref[2 * k], at, LANES // 2 + at)
                stage(odd, x, ref[f * there.astype(jnp.int32), x], masks_ref[k], outside, start)

    def predict_inner(f, odd):
        total = jnp.zeros((8, shots), jnp.float32)
        for block in range(1, blocks - 1):
            total = total + predict(f, odd, block)
        inner_ref[f] = lanes_of(total)

    def predict_outer(f, odd):
        total = jnp.zeros((8, shots), jnp.float32)
        for block in sorted({0, blocks - 1}):
            total = total + predict(f, odd, block)
        outer_ref[f] = lanes_of(total)

    def flood(n):
        for there, peer in near:
            @pl.when(there)
            def _():
                pl.semaphore_signal(flood_sem.at[n], inc=1, device_id=peer, device_id_type=MESH)

    def step(f, odd):
        @pl.when(f > 0)
        def _():
            pl.semaphore_wait(flood_sem.at[f - 1], beside)

        flood(f)
        wait_halos(f)
        stage_halos(f, odd)
        stage_own(f + 1, 1 - odd)
        predict_outer(f, odd)
        predict_inner(f + 1, 1 - odd)

    wait_edges(0)
    stage_own(0, 0)
    prepare(1, 1)
    predict_inner(0, 0)

    @pl.when(has_above)
    def _():
        mask_copy(0).wait_recv()

    @pl.when(has_below)
    def _():
        mask_copy(1).wait_recv()

    for i, there, came, peer, end in corners:
        @pl.when(came)
        def _():
            corner_copy(i, peer, end).wait_recv()

    @pl.loop(0, slices // 2 - 1)
    def _(pair):
        f = 2 * pair
        step(f, 0)
        prepare(f + 2, 0)
        for g in range(1, GROUPS):
            @pl.when(f + 2 == g * group)
            def _():
                wait_edges(g)

        step(f + 1, 1)
        prepare(f + 3, 1)

    step(slices - 2, 0)
    pl.semaphore_wait(flood_sem.at[slices - 2], beside)
    wait_halos(slices - 1)
    stage_halos(slices - 1, 1)
    predict_outer(slices - 1, 1)
    for n in range(slices - 1, flood_sem.shape[0]):
        flood(n)
        pl.semaphore_wait(flood_sem.at[n], beside)

    cells = jnp.concatenate([jnp.sum(data_ref[...], axis=1), jnp.sum(inner_ref[...] + outer_ref[...], axis=1)], axis=0)
    row = lax.broadcasted_iota(jnp.int32, cells.shape, 0)
    col = lax.broadcasted_iota(jnp.int32, cells.shape, 1)
    spot = jnp.where(row < slices, row, row - slices + LANES // 2)
    cells = jnp.where(col == spot, jnp.sum(cells, axis=1, keepdims=True), 0.0)
    mine = jnp.sum(cells, axis=0, keepdims=True)
    mine_ref[...] = mine

    def exchange(source, target, pairs, send, recv):
        copies = []
        for n, (a, b) in enumerate(pairs):
            copy = pltpu.make_async_remote_copy(
                src_ref=source, dst_ref=target.at[n], send_sem=send.at[n], recv_sem=recv.at[n],
                device_id=peer_of(a, b), device_id_type=MESH,
            )
            copy.start()
            copies.append(copy)
        for copy in copies:
            copy.wait()

    if direct:
        pairs = [(a, b) for b in range(fast_count) for a in range(slow_count) if a or b]
        exchange(mine_ref, space_ref, pairs, send_b, recv_b)
        total = mine + jnp.sum(space_ref[...], axis=0)
    else:
        exchange(mine_ref, plane_ref, [(a, 0) for a in range(1, slow_count)], send_a, recv_a)
        total = mine + jnp.sum(plane_ref[...], axis=0)
        mine_ref[...] = total
        exchange(mine_ref, space_ref, [(0, b) for b in range(1, fast_count)], send_b, recv_b)
        total = total + jnp.sum(space_ref[...], axis=0)
    gain_ref[...] = jnp.sqrt((total + 1e-06) / (pltpu.roll(total, LANES // 2, 1) + 1e-06))

    @pl.when(has_below)
    def _():
        mask_copy(0).wait_send()

        @pl.loop(0, slices)
        def _(f):
            up(f).wait_send()

    @pl.when(has_above)
    def _():
        mask_copy(1).wait_send()

        @pl.loop(0, slices)
        def _(f):
            down(f).wait_send()

    for g in range(GROUPS):
        @pl.when(has_next)
        def _():
            edge_copy(g, 0).wait_send()

        @pl.when(has_prev)
        def _():
            edge_copy(g, 1).wait_send()

    for i, there, came, peer, end in corners:
        @pl.when(there)
        def _():
            corner_copy(i, peer, end).wait_send()


def forward(axes, wave, band, shift, live, taper):
    _, slices, receivers, shots = wave.shape
    slow_count, fast_count = axes[0][1], axes[1][1]
    direct = slow_count * fast_count <= 32
    peers = slow_count * fast_count - 1 if direct else fast_count - 1
    farthest = slow_count + fast_count - 2 if direct else max(slow_count, fast_count) - 1
    tall = receivers + DEPTH - HALF
    blocks, quarters = receivers // BLOCK, LANES // (4 * slices // GROUPS)
    packed = -(-blocks // quarters) * BLOCK
    dma = pltpu.SemaphoreType.DMA
    whole = pl.BlockSpec(memory_space=pltpu.VMEM)
    hbm = pl.BlockSpec(memory_space=pltpu.HBM)
    return pl.pallas_call(
        functools.partial(forward_kernel, axes),
        in_specs=[hbm] * 5,
        out_specs=[whole, whole, whole],
        out_shape=[
            jax.ShapeDtypeStruct(wave.shape, jnp.float32),
            jax.ShapeDtypeStruct(wave.shape, jnp.float32),
            jax.ShapeDtypeStruct((1, LANES), jnp.float32),
        ],
        scratch_shapes=[
            pltpu.SMEM(shift.shape, jnp.int32),
            pltpu.SMEM(taper.shape, jnp.float32),
            pltpu.SMEM(live.shape, jnp.int32),
            pltpu.VMEM((receivers, LANES), jnp.float32),
            pltpu.VMEM(band.shape, jnp.float32),
            pltpu.VMEM((4 * LANES, 2 * LANES), jnp.bfloat16),
            *[pltpu.VMEM((receivers // HALF, 2, 2, HALF, DEPTH), jnp.bfloat16)] * 2,
            *[pltpu.VMEM((2, tall, shots), jnp.bfloat16)] * 4,
            pltpu.VMEM((slices, 2, HALO, shots), jnp.float32),
            pltpu.VMEM((slices, 2, HALO, shots), jnp.float32),
            pltpu.VMEM((GROUPS, 2, packed, LANES), jnp.float32),
            pltpu.VMEM((GROUPS, packed, LANES), jnp.float32),
            pltpu.VMEM((GROUPS, packed, LANES), jnp.float32),
            pltpu.VMEM((2, HALO, LANES), jnp.float32),
            pltpu.VMEM((4, HALO, LANES), jnp.float32),
            pltpu.VMEM((2, HALO, LANES), jnp.float32),
            *[pltpu.VMEM((slices, 8, LANES), jnp.float32)] * 3,
            pltpu.VMEM((1, LANES), jnp.float32),
            pltpu.VMEM((slow_count - 1, 1, LANES), jnp.float32),
            pltpu.VMEM((peers, 1, LANES), jnp.float32),
            dma((slices,)), dma((4,)), dma((slices,)), dma((slices,)), dma((slices,)), dma((slices,)),
            dma((2,)), dma((2,)), dma((GROUPS, 2)), dma((GROUPS, 2)), dma((4,)), dma((4,)),
            dma((slow_count - 1,)), dma((slow_count - 1,)), dma((peers,)), dma((peers,)),
            pltpu.SemaphoreType.REGULAR((max(slices, farthest) - 1,)),
        ],
        cost_estimate=pl.CostEstimate(flops=2**33, bytes_accessed=wave.size * 8, transcendentals=0),
        compiler_params=pltpu.CompilerParams(
            collective_id=1, has_side_effects=True, vmem_limit_bytes=14 * 2**20
        ),
        name="forward",
    )(shift, taper, live, wave, band)


def finish_kernel(gain_ref, wave_ref, mult_ref, mult_hbm, prim_hbm, prim_ref, mult_sem, prim_sem):
    slices = wave_ref.shape[1]
    slots = prim_ref.shape[0]

    def mult_copy(f):
        return pltpu.make_async_copy(mult_ref.at[:, f], mult_hbm.at[:, f], mult_sem.at[f])

    def prim_copy(f):
        return pltpu.make_async_copy(prim_ref.at[lax.rem(f, slots)], prim_hbm.at[:, f], prim_sem.at[f])

    col = lax.broadcasted_iota(jnp.int32, (1, LANES), 1)

    @pl.loop(0, slices)
    def _(f):
        mult_copy(f).start()
        gain = jnp.sum(jnp.where(col == f, gain_ref[...], 0.0))

        @pl.when(f >= slots)
        def _():
            prim_copy(f - slots).wait()

        for x in range(2):
            for r in range(0, wave_ref.shape[2], BLOCK):
                rows = pl.ds(r, BLOCK)
                prim_ref[lax.rem(f, slots), x, rows, :] = wave_ref[x, f, rows, :] - gain * mult_ref[x, f, rows, :]
        prim_copy(f).start()

    @pl.loop(0, slices)
    def _(f):
        mult_copy(f).wait()

    @pl.loop(max(slices - slots, 0), slices)
    def _(f):
        prim_copy(f).wait()


def finish(gain, wave, mult):
    slices = wave.shape[1]
    whole = pl.BlockSpec(memory_space=pltpu.VMEM)
    hbm = pl.BlockSpec(memory_space=pl.ANY)
    return pl.pallas_call(
        finish_kernel,
        in_specs=[whole, whole, whole],
        out_specs=[hbm, hbm],
        out_shape=[jax.ShapeDtypeStruct(wave.shape, jnp.float32)] * 2,
        scratch_shapes=[
            pltpu.VMEM((min(SLOTS, slices), 2, *wave.shape[2:]), jnp.float32),
            pltpu.SemaphoreType.DMA((slices,)),
            pltpu.SemaphoreType.DMA((slices,)),
        ],
        cost_estimate=pl.CostEstimate(flops=wave.size * 2, bytes_accessed=wave.size * 8, transcendentals=0),
        compiler_params=pltpu.CompilerParams(vmem_limit_bytes=12 * 2**20),
        name="finish",
    )(gain, wave, mult)


def per_device(wavefield, surface_band, band_shift, trace_mask, shot_taper):
    axes = (("src", lax.axis_size("src")), ("rcv", lax.axis_size("rcv")))
    def keep(array):
        return pltpu.with_memory_space_constraint(array, pltpu.HBM) if array.size > 1 else array

    small = [keep(array) for array in (surface_band, band_shift, trace_mask, shot_taper)]
    wave, mult, gain = forward(axes, wavefield, *small)
    return tuple(finish(gain, wave, mult))


def solution(mesh):
    in_specs = (P(None, None, "rcv", "src"), P(None, "rcv", None), P("rcv"), P("rcv"), P())
    out_specs = (P(None, None, "rcv", "src"), P(None, None, "rcv", "src"))
    return jax.shard_map(
        per_device, mesh=mesh, in_specs=in_specs, out_specs=out_specs, check_vma=False
    )
```

```python
import functools

import jax
import jax.numpy as jnp
from jax import lax
from jax.experimental import pallas as pl
from jax.experimental.pallas import tpu as pltpu
from jax.sharding import PartitionSpec as P

APER = 64
SHIFT = 16
BLOCK = 64
HALF = BLOCK // 2
SHALF = 2
LANES = 128
DEPTH = 128
HALO = APER // 2 + SHIFT
FIRST = 2
GROUPS = 2
STRIP = 16
SLOTS = 8
MESH = pl.DeviceIdType.MESH


def split(cells):
    high = cells.astype(jnp.bfloat16)
    low = (cells - high.astype(jnp.float32)).astype(jnp.bfloat16)
    return high, low


def forward_kernel(axes, shift_hbm, taper_hbm, live_hbm, wave_hbm, band_hbm, *refs):
    wave_ref, mult_ref, gain_ref = refs[:3]
    (
        shift_ref, taper_ref, live_ref, mask_ref, band_ref, turn_ref,
        even_weight, odd_weight, even_high, odd_high, even_low, odd_low, above_ref, below_ref, edge_ref, next_ref, prev_ref, ends_ref, corner_ref, masks_ref, line_ref, came_ref,
        data_ref, inner_ref, outer_ref, mine_ref, plane_ref, space_ref,
        load_sem, small_sem, send_up, recv_up, send_down, recv_down, send_mask, recv_mask,
        send_edge, recv_edge, send_corner, recv_corner, send_a, recv_a, send_b, recv_b, flood_sem,
    ) = refs[3:]
    (slow, slow_count), (fast, fast_count) = axes
    slow_me, fast_me = lax.axis_index(slow), lax.axis_index(fast)
    _, slices, receivers, shots = wave_ref.shape
    blocks, group = receivers // BLOCK, slices // GROUPS
    share = 4 * group
    quarters = LANES // share
    has_above, has_below = fast_me > 0, fast_me < fast_count - 1
    has_prev, has_next = slow_me > 0, slow_me < slow_count - 1
    direct = slow_count * fast_count <= 32

    def peer_of(a, b):
        return {slow: lax.rem(slow_me + a, slow_count), fast: lax.rem(fast_me + b, fast_count)}

    corners = []
    for i, (down, right) in enumerate([(1, 1), (1, -1), (-1, 1), (-1, -1)]):
        there = (has_below if down > 0 else has_above) & (has_next if right > 0 else has_prev)
        came = (has_above if down > 0 else has_below) & (has_prev if right > 0 else has_next)
        corners.append((i, there, came, {fast: fast_me + down, slow: slow_me + right}, 0 if down > 0 else 1))

    spans = [(0, LANES), (shots - LANES, LANES), (LANES, shots - 2 * LANES)]
    spans = [pl.ds(start, count) for start, count in spans if count > 0]

    def load(f, part):
        cells = (slice(None), f, slice(None), spans[part])
        return pltpu.make_async_copy(wave_hbm.at[cells], wave_ref.at[cells], load_sem.at[part, f])

    def wait_rest(f):
        for part in range(2, len(spans)):
            load(f, part).wait()

    def up(f):
        return pltpu.make_async_remote_copy(
            src_ref=wave_hbm.at[:, f, pl.ds(receivers - HALO, HALO)], dst_ref=above_ref.at[f],
            send_sem=send_up.at[f], recv_sem=recv_up.at[f],
            device_id={fast: fast_me + 1}, device_id_type=MESH,
        )

    def down(f):
        return pltpu.make_async_remote_copy(
            src_ref=wave_hbm.at[:, f, pl.ds(0, HALO)], dst_ref=below_ref.at[f],
            send_sem=send_down.at[f], recv_sem=recv_down.at[f],
            device_id={fast: fast_me - 1}, device_id_type=MESH,
        )

    def mask_copy(i):
        return pltpu.make_async_remote_copy(
            src_ref=line_ref.at[i], dst_ref=came_ref.at[i],
            send_sem=send_mask.at[i], recv_sem=recv_mask.at[i],
            device_id={fast: fast_me - 1 if i else fast_me + 1}, device_id_type=MESH,
        )

    def edge_copy(g, i):
        return pltpu.make_async_remote_copy(
            src_ref=edge_ref.at[g, 1 - i], dst_ref=next_ref.at[g] if i else prev_ref.at[g],
            send_sem=send_edge.at[g, i], recv_sem=recv_edge.at[g, i],
            device_id={slow: slow_me - 1 if i else slow_me + 1}, device_id_type=MESH,
        )

    def corner_copy(i, peer, end):
        return pltpu.make_async_remote_copy(
            src_ref=ends_ref.at[end, 1 - i % 2], dst_ref=corner_ref.at[i],
            send_sem=send_corner.at[i], recv_sem=recv_corner.at[i],
            device_id=peer, device_id_type=MESH,
        )

    def send_halos(f):
        @pl.when(has_below)
        def _():
            up(f).start()

        @pl.when(has_above)
        def _():
            down(f).start()

    small = [
        pltpu.make_async_copy(a, b, small_sem.at[i])
        for i, (a, b) in enumerate(
            [(live_hbm, live_ref), (taper_hbm, taper_ref), (shift_hbm, shift_ref), (band_hbm, band_ref)]
        )
    ]
    for copy in small[:3]:
        copy.start()
    barrier = pltpu.get_barrier_semaphore()
    near = [
        (has_above, {fast: fast_me - 1}), (has_below, {fast: fast_me + 1}),
        (has_prev, {slow: slow_me - 1}), (has_next, {slow: slow_me + 1}),
    ]
    beside = sum(there.astype(jnp.int32) for there, _ in near)
    greeted = beside + sum(there.astype(jnp.int32) for _, there, *_ in corners)
    for there, peer in near + [(there, peer) for _, there, _, peer, _ in corners]:
        @pl.when(there)
        def _():
            pl.semaphore_signal(barrier, inc=1, device_id=peer, device_id_type=MESH)

    small[3].start()

    for parts in (range(2), range(2, len(spans))):
        @pl.loop(0, slices)
        def _(f):
            for part in parts:
                load(f, part).start()

    pl.semaphore_wait(barrier, greeted)

    for f in range(FIRST):
        send_halos(f)

    small[0].wait()
    line = lax.broadcasted_iota(jnp.int32, (8, LANES), 0)

    @pl.loop(0, receivers // 8, unroll=4)
    def _(i):
        cells = jnp.zeros((8, LANES), jnp.float32)
        for r in range(8):
            cells = jnp.where(line == r, live_ref[i * 8 + r].astype(jnp.float32), cells)
        mask_ref[pl.ds(pl.multiple_of(i * 8, 8), 8), :] = cells

    diagonal = lax.broadcasted_iota(jnp.int32, (HALO, LANES), 0) == lax.broadcasted_iota(jnp.int32, (HALO, LANES), 1)
    for i, start in enumerate((receivers - HALO, 0)):
        cells = jnp.where(diagonal, mask_ref[start : start + HALO, :], 0.0)
        line_ref[i] = jnp.sum(cells, axis=0, keepdims=True)

    @pl.when(has_below)
    def _():
        mask_copy(0).start()

    @pl.when(has_above)
    def _():
        mask_copy(1).start()

    small[1].wait()
    small[2].wait()

    source = lax.broadcasted_iota(jnp.int32, (2 * LANES, LANES), 0)
    source = jnp.where(source < LANES, source, jnp.where(source < LANES + LANES // 2, source, source - 2 * LANES))
    offset = source - lax.broadcasted_iota(jnp.int32, (2 * LANES, LANES), 1) + SHALF
    turn = jnp.zeros((2 * LANES, LANES), jnp.float32)
    for u in range(2 * SHALF + 1):
        turn = jnp.where(offset == u, taper_ref[u], turn)
    turn = jnp.concatenate(split(turn), axis=1)
    for i in range(2):
        turn_ref[2 * i * LANES : 2 * (i + 1) * LANES, :] = turn

    rows_refs, weight_refs = ((even_high, even_low), (odd_high, odd_low)), (even_weight, odd_weight)
    for there, ref in ((has_prev, prev_ref), (has_next, next_ref)):
        @pl.when(jnp.logical_not(there))
        def _():
            ref[...] = jnp.zeros_like(ref)

    for i, there, came, peer, end in corners:
        @pl.when(jnp.logical_not(came))
        def _():
            corner_ref[i] = jnp.zeros(corner_ref.shape[1:], jnp.float32)

    for i, (there, ref) in enumerate(((has_above, above_ref), (has_below, below_ref))):
        @pl.when(jnp.logical_not(there))
        def _():
            came_ref[i] = jnp.zeros(came_ref.shape[1:], jnp.float32)
            ref[0] = jnp.zeros(ref.shape[1:], jnp.float32)

    edge_ref[...] = jnp.zeros_like(edge_ref)

    column = lax.broadcasted_iota(jnp.int32, (BLOCK, LANES), 1)

    def prepare(f, odd):
        weight_ref = weight_refs[odd]
        live = (column // APER) == odd
        lanes = pl.ds(pl.multiple_of(f // 2 * LANES, LANES), LANES)
        for block in range(blocks):
            for x in range(2):
                cells = jnp.where(live, band_ref[x, block * BLOCK : (block + 1) * BLOCK, lanes], 0.0)
                cells = pltpu.roll(cells, shift_ref[block] + SHIFT + APER * odd, 1)
                for h in range(2):
                    taps = pltpu.roll(cells[h * HALF : (h + 1) * HALF], 0, 1, stride=1, stride_axis=0)
                    weight_ref[2 * block + h, 0, x], weight_ref[2 * block + h, 1, x] = split(taps)

    small[3].wait()
    prepare(0, 0)

    lane = lax.broadcasted_iota(jnp.int32, (BLOCK, LANES), 1)

    def packed(block):
        return pl.ds(block // quarters * BLOCK, BLOCK), block % quarters * share

    for g in range(GROUPS):
        @pl.loop(0, group, unroll=2)
        def _(i):
            f = g * group + i
            load(f, 0).wait()
            load(f, 1).wait()
            for chunk in range(0, blocks, quarters):
                rows, _ = packed(chunk)
                first, last = edge_ref[g, 0, rows, :], edge_ref[g, 1, rows, :]
                for block in range(chunk, min(chunk + quarters, blocks)):
                    cells = pl.ds(block * BLOCK, BLOCK)
                    for x in range(2):
                        place = packed(block)[1] + 4 * i + 2 * x
                        ours = (lane >= place) & (lane < place + 2)
                        first = jnp.where(ours, pltpu.roll(wave_ref[x, f, cells, :LANES], place, 1), first)
                        turned = pltpu.roll(wave_ref[x, f, cells, shots - LANES :], lax.rem(place + 2, LANES), 1)
                        last = jnp.where(ours, turned, last)
                edge_ref[g, 0, rows, :] = first
                edge_ref[g, 1, rows, :] = last

        @pl.when(has_next)
        def _():
            edge_copy(g, 0).start()

        @pl.when(has_prev)
        def _():
            edge_copy(g, 1).start()

    fold = HALO // 2
    wide = lax.broadcasted_iota(jnp.int32, (HALO, LANES), 1)
    for end, block, skip in ((0, blocks - 1, BLOCK - HALO), (1, 0, 0)):
        rows, place = packed(block)
        for side in range(2):
            cells = jnp.zeros((HALO, LANES), jnp.float32)
            for g in range(GROUPS):
                part = pltpu.roll(edge_ref[g, side, rows, :][skip : skip + HALO], (g * share - place) % LANES, 1)
                cells = jnp.where((wide >= g * share) & (wide < (g + 1) * share), part, cells)
            ends_ref[end, side] = jnp.where(
                wide[:fold] < LANES // 2, cells[:fold], pltpu.roll(cells[fold:], LANES // 2, 1)
            )

    for i, there, came, peer, end in corners:
        @pl.when(there)
        def _():
            corner_copy(i, peer, end).start()

    @pl.loop(FIRST, slices)
    def _(f):
        send_halos(f)

    def turned(after, before, at_after, at_before):
        count = after.shape[0]
        after = pltpu.roll(after, lax.rem(LANES - at_after, LANES), 1)
        before = pltpu.roll(before, lax.rem(2 * LANES - 2 - at_before, LANES), 1)
        return jnp.where(lax.broadcasted_iota(jnp.int32, (count, LANES), 1) < LANES // 2, after, before)

    def stage(odd, x, wave, mask, outside, at):
        high_ref, low_ref = rows_refs[odd]
        count = wave.shape[0]
        tile = lax.broadcasted_iota(jnp.int32, (count, LANES), 1) < LANES // 2
        outside = split(outside * mask)
        inside = [split(wave[:, i * LANES : (i + 1) * LANES] * mask) for i in range(shots // LANES)]
        cells = [outside, *inside, outside]
        parts = []
        for part in range(2):
            rows = []
            for i in range(shots // LANES):
                around = jnp.where(tile, cells[i + 2][part], cells[i][part])
                rows.append(jnp.concatenate([cells[i + 1][part], around], axis=1))
            parts.append(jnp.concatenate(rows, axis=0))
        both = jnp.dot(jnp.concatenate(parts, axis=1), turn_ref[...], preferred_element_type=jnp.float32)
        high, low = split(both[:, :LANES] + both[:, LANES:])
        rows = pl.ds(at, count)
        for i in range(shots // LANES):
            lanes = pl.ds(i * LANES, LANES)
            high_ref[x, rows, lanes] = high[i * count : (i + 1) * count]
            low_ref[x, rows, lanes] = low[i * count : (i + 1) * count]

    def predict(f, odd, block):
        (high_ref, low_ref), weight_ref = rows_refs[odd], weight_refs[odd]
        total = jnp.zeros((8, shots), jnp.float32)
        for h in range(2):
            half = 2 * block + h
            base = half * HALF
            parts = []
            for part in range(2):
                real, imag = weight_ref[half, part, 0], weight_ref[half, part, 1]
                parts.append(jnp.concatenate([real, -imag], axis=1))
                parts.append(jnp.concatenate([imag, real], axis=1))
            window = pl.ds(base, DEPTH)
            high = jnp.concatenate([high_ref[x, window, :] for x in range(2)], axis=0)
            low = jnp.concatenate([low_ref[x, window, :] for x in range(2)], axis=0)
            upper = jnp.dot(jnp.concatenate(parts, axis=0), high, preferred_element_type=jnp.float32)
            lower = jnp.dot(jnp.concatenate(parts[:2], axis=0), low, preferred_element_type=jnp.float32)
            pred = upper[:BLOCK] + (upper[BLOCK:] + lower)
            for x in range(2):
                mult_ref[x, f, pl.ds(base, HALF), :] = pred[x * HALF : (x + 1) * HALF]
            total = total + jnp.sum((pred * pred).reshape(-1, 8, shots), axis=0)
        return total

    def lanes_of(total):
        return sum(total[:, i * LANES : (i + 1) * LANES] for i in range(shots // LANES))

    def wait_edges(g):
        @pl.when(has_prev)
        def _():
            edge_copy(g, 0).wait_recv()

        @pl.when(has_next)
        def _():
            edge_copy(g, 1).wait_recv()

    def wait_halos(f, sides=(0, 1)):
        for side in sides:
            @pl.when(has_below if side else has_above)
            def _():
                (down if side else up)(f).wait_recv()

    def stage_own(f, odd):
        g, i = f // group, lax.rem(f, group)
        data = jnp.zeros((8, LANES), jnp.float32)
        for block in range(blocks):
            rows = pl.ds(block * BLOCK, BLOCK)
            cells, place = packed(block)
            after, before = next_ref[g, cells, :], prev_ref[g, cells, :]
            for x in range(2):
                wave = wave_ref[x, f, rows, :]
                at = place + 4 * i + 2 * x
                stage(odd, x, wave, mask_ref[rows, :], turned(after, before, at, at), block * BLOCK + HALO)
                data = data + lanes_of(jnp.sum((wave * wave).reshape(-1, 8, shots), axis=0))
        data_ref[f] = data

    def stage_halos(f, odd, sides=(0, 1)):
        for x in range(2):
            at = 4 * f + 2 * x
            for k in sides:
                ref, start, there = ((above_ref, 0, has_above), (below_ref, HALO + receivers, has_below))[k]
                ends = [turned(corner_ref[2 * k + 1], corner_ref[2 * k], at + c, at + c) for c in (0, LANES // 2)]
                outside = jnp.concatenate(ends, axis=0)
                stage(odd, x, ref[f * there.astype(jnp.int32), x], masks_ref[k], outside, start)

    def predict_inner(f, odd):
        total = jnp.zeros((8, shots), jnp.float32)
        for block in range(1, blocks - 1):
            total = total + predict(f, odd, block)
        inner_ref[f] = lanes_of(total)

    def predict_outer(f, odd):
        total = jnp.zeros((8, shots), jnp.float32)
        for block in sorted({0, blocks - 1}):
            total = total + predict(f, odd, block)
        outer_ref[f] = lanes_of(total)

    def flood(n):
        for there, peer in near:
            @pl.when(there)
            def _():
                pl.semaphore_signal(flood_sem.at[n], inc=1, device_id=peer, device_id_type=MESH)

    def step(f, odd):
        @pl.when(f > 0)
        def _():
            pl.semaphore_wait(flood_sem.at[f - 1], beside)

        flood(f)
        wait_rest(f + 1)
        wait_halos(f)
        stage_halos(f, odd)
        stage_own(f + 1, 1 - odd)
        predict_outer(f, odd)
        predict_inner(f + 1, 1 - odd)

    wait_edges(0)
    wait_rest(0)
    stage_own(0, 0)
    prepare(1, 1)
    predict_inner(0, 0)

    @pl.when(has_above)
    def _():
        mask_copy(0).wait_recv()

    @pl.when(has_below)
    def _():
        mask_copy(1).wait_recv()

    for i, there, came, peer, end in corners:
        @pl.when(came)
        def _():
            corner_copy(i, peer, end).wait_recv()

    for i in range(2):
        cells = jnp.sum(jnp.where(diagonal, came_ref[i], 0.0), axis=1, keepdims=True)
        masks_ref[i] = jnp.broadcast_to(cells, masks_ref.shape[1:])

    @pl.loop(0, slices // 2 - 1)
    def _(pair):
        f = 2 * pair
        step(f, 0)
        prepare(f + 2, 0)
        for g in range(1, GROUPS):
            @pl.when(f + 2 == g * group)
            def _():
                wait_edges(g)

        step(f + 1, 1)
        prepare(f + 3, 1)

    step(slices - 2, 0)
    pl.semaphore_wait(flood_sem.at[slices - 2], beside)

    last = slices - 1
    outer_ref[last] = jnp.zeros((8, LANES), jnp.float32)
    cells = jnp.concatenate([jnp.sum(data_ref[...], axis=1), jnp.sum(inner_ref[...] + outer_ref[...], axis=1)], axis=0)
    row = lax.broadcasted_iota(jnp.int32, cells.shape, 0)
    col = lax.broadcasted_iota(jnp.int32, cells.shape, 1)
    spot = jnp.where(row < slices, row, row - slices + LANES // 2)
    cells = jnp.where(col == spot, jnp.sum(cells, axis=1, keepdims=True), 0.0)
    mine_ref[...] = jnp.sum(cells, axis=0, keepdims=True)

    if blocks > 1:
        for parity, sides in ((0, (1, 0)), (1, (0, 1))):
            @pl.when(lax.rem(fast_me, 2) == parity)
            def _():
                for side in sides:
                    wait_halos(last, (side,))
                    stage_halos(last, 1, (side,))
                    outer_ref[last] += lanes_of(predict(last, 1, (blocks - 1) * side))
    else:
        wait_halos(last)
        stage_halos(last, 1)
        predict_outer(last, 1)
    for n in range(slices - 1, flood_sem.shape[0]):
        flood(n)
        pl.semaphore_wait(flood_sem.at[n], beside)

    tail = jnp.sum(jnp.sum(outer_ref[last], axis=0, keepdims=True), axis=1, keepdims=True)
    spot = lax.broadcasted_iota(jnp.int32, (1, LANES), 1) == LANES // 2 + last
    mine = mine_ref[...] + jnp.where(spot, tail, 0.0)
    mine_ref[...] = mine

    def exchange(source, target, pairs, send, recv):
        copies = []
        for n, (a, b) in enumerate(pairs):
            copy = pltpu.make_async_remote_copy(
                src_ref=source, dst_ref=target.at[n], send_sem=send.at[n], recv_sem=recv.at[n],
                device_id=peer_of(a, b), device_id_type=MESH,
            )
            copy.start()
            copies.append(copy)
        for copy in copies:
            copy.wait()

    if direct:
        pairs = [(a, b) for b in range(fast_count) for a in range(slow_count) if a or b]
        exchange(mine_ref, space_ref, pairs, send_b, recv_b)
        total = mine + jnp.sum(space_ref[...], axis=0)
    else:
        exchange(mine_ref, plane_ref, [(a, 0) for a in range(1, slow_count)], send_a, recv_a)
        total = mine + jnp.sum(plane_ref[...], axis=0)
        mine_ref[...] = total
        exchange(mine_ref, space_ref, [(0, b) for b in range(1, fast_count)], send_b, recv_b)
        total = total + jnp.sum(space_ref[...], axis=0)
    gain_ref[...] = jnp.sqrt((total + 1e-06) / (pltpu.roll(total, LANES // 2, 1) + 1e-06))

    @pl.when(has_below)
    def _():
        mask_copy(0).wait_send()

        @pl.loop(0, slices)
        def _(f):
            up(f).wait_send()

    @pl.when(has_above)
    def _():
        mask_copy(1).wait_send()

        @pl.loop(0, slices)
        def _(f):
            down(f).wait_send()

    for g in range(GROUPS):
        @pl.when(has_next)
        def _():
            edge_copy(g, 0).wait_send()

        @pl.when(has_prev)
        def _():
            edge_copy(g, 1).wait_send()

    for i, there, came, peer, end in corners:
        @pl.when(there)
        def _():
            corner_copy(i, peer, end).wait_send()


def forward(axes, wave, band, shift, live, taper):
    _, slices, receivers, shots = wave.shape
    slow_count, fast_count = axes[0][1], axes[1][1]
    direct = slow_count * fast_count <= 32
    peers = slow_count * fast_count - 1 if direct else fast_count - 1
    farthest = slow_count + fast_count - 2 if direct else max(slow_count, fast_count) - 1
    tall = receivers + DEPTH - HALF
    blocks, quarters = receivers // BLOCK, LANES // (4 * slices // GROUPS)
    packed = -(-blocks // quarters) * BLOCK
    dma = pltpu.SemaphoreType.DMA
    whole = pl.BlockSpec(memory_space=pltpu.VMEM)
    hbm = pl.BlockSpec(memory_space=pltpu.HBM)
    return pl.pallas_call(
        functools.partial(forward_kernel, axes),
        in_specs=[hbm] * 5,
        out_specs=[whole, whole, whole],
        out_shape=[
            jax.ShapeDtypeStruct(wave.shape, jnp.float32),
            jax.ShapeDtypeStruct(wave.shape, jnp.float32),
            jax.ShapeDtypeStruct((1, LANES), jnp.float32),
        ],
        scratch_shapes=[
            pltpu.SMEM(shift.shape, jnp.int32),
            pltpu.SMEM(taper.shape, jnp.float32),
            pltpu.SMEM(live.shape, jnp.int32),
            pltpu.VMEM((receivers, LANES), jnp.float32),
            pltpu.VMEM(band.shape, jnp.float32),
            pltpu.VMEM((4 * LANES, 2 * LANES), jnp.bfloat16),
            *[pltpu.VMEM((receivers // HALF, 2, 2, HALF, DEPTH), jnp.bfloat16)] * 2,
            *[pltpu.VMEM((2, tall, shots), jnp.bfloat16)] * 4,
            pltpu.VMEM((slices, 2, HALO, shots), jnp.float32),
            pltpu.VMEM((slices, 2, HALO, shots), jnp.float32),
            pltpu.VMEM((GROUPS, 2, packed, LANES), jnp.float32),
            pltpu.VMEM((GROUPS, packed, LANES), jnp.float32),
            pltpu.VMEM((GROUPS, packed, LANES), jnp.float32),
            pltpu.VMEM((2, 2, HALO // 2, LANES), jnp.float32),
            pltpu.VMEM((4, HALO // 2, LANES), jnp.float32),
            pltpu.VMEM((2, HALO, LANES), jnp.float32),
            pltpu.VMEM((2, 1, LANES), jnp.float32),
            pltpu.VMEM((2, 1, LANES), jnp.float32),
            *[pltpu.VMEM((slices, 8, LANES), jnp.float32)] * 3,
            pltpu.VMEM((1, LANES), jnp.float32),
            pltpu.VMEM((slow_count - 1, 1, LANES), jnp.float32),
            pltpu.VMEM((peers, 1, LANES), jnp.float32),
            dma((3, slices)), dma((4,)), dma((slices,)), dma((slices,)), dma((slices,)), dma((slices,)),
            dma((2,)), dma((2,)), dma((GROUPS, 2)), dma((GROUPS, 2)), dma((4,)), dma((4,)),
            dma((slow_count - 1,)), dma((slow_count - 1,)), dma((peers,)), dma((peers,)),
            pltpu.SemaphoreType.REGULAR((max(slices, farthest) - 1,)),
        ],
        cost_estimate=pl.CostEstimate(flops=2**33, bytes_accessed=wave.size * 8, transcendentals=0),
        compiler_params=pltpu.CompilerParams(
            collective_id=1, has_side_effects=True, vmem_limit_bytes=14 * 2**20
        ),
        name="forward",
    )(shift, taper, live, wave, band)


def finish_kernel(gain_ref, wave_ref, mult_ref, mult_hbm, prim_hbm, prim_ref, mult_sem, prim_sem):
    slices = wave_ref.shape[1]
    slots = prim_ref.shape[0]

    def mult_copy(f):
        return pltpu.make_async_copy(mult_ref.at[:, f], mult_hbm.at[:, f], mult_sem.at[f])

    def prim_copy(f):
        return pltpu.make_async_copy(prim_ref.at[lax.rem(f, slots)], prim_hbm.at[:, f], prim_sem.at[f])

    col = lax.broadcasted_iota(jnp.int32, (1, LANES), 1)

    @pl.loop(0, slices)
    def _(f):
        mult_copy(f).start()
        gain = jnp.sum(jnp.where(col == f, gain_ref[...], 0.0))

        @pl.when(f >= slots)
        def _():
            prim_copy(f - slots).wait()

        for x in range(2):
            for r in range(0, wave_ref.shape[2], BLOCK):
                rows = pl.ds(r, BLOCK)
                prim_ref[lax.rem(f, slots), x, rows, :] = wave_ref[x, f, rows, :] - gain * mult_ref[x, f, rows, :]
        prim_copy(f).start()

    @pl.loop(0, slices)
    def _(f):
        mult_copy(f).wait()

    @pl.loop(max(slices - slots, 0), slices)
    def _(f):
        prim_copy(f).wait()


def finish(gain, wave, mult):
    slices = wave.shape[1]
    whole = pl.BlockSpec(memory_space=pltpu.VMEM)
    hbm = pl.BlockSpec(memory_space=pl.ANY)
    return pl.pallas_call(
        finish_kernel,
        in_specs=[whole, whole, whole],
        out_specs=[hbm, hbm],
        out_shape=[jax.ShapeDtypeStruct(wave.shape, jnp.float32)] * 2,
        scratch_shapes=[
            pltpu.VMEM((min(SLOTS, slices), 2, *wave.shape[2:]), jnp.float32),
            pltpu.SemaphoreType.DMA((slices,)),
            pltpu.SemaphoreType.DMA((slices,)),
        ],
        cost_estimate=pl.CostEstimate(flops=wave.size * 2, bytes_accessed=wave.size * 8, transcendentals=0),
        compiler_params=pltpu.CompilerParams(vmem_limit_bytes=12 * 2**20),
        name="finish",
    )(gain, wave, mult)


def per_device(wavefield, surface_band, band_shift, trace_mask, shot_taper):
    axes = (("src", lax.axis_size("src")), ("rcv", lax.axis_size("rcv")))
    def keep(array):
        return pltpu.with_memory_space_constraint(array, pltpu.HBM) if array.size > 1 else array

    small = [keep(array) for array in (surface_band, band_shift, trace_mask, shot_taper)]
    wave, mult, gain = forward(axes, wavefield, *small)
    return tuple(finish(gain, wave, mult))


def solution(mesh):
    in_specs = (P(None, None, "rcv", "src"), P(None, "rcv", None), P("rcv"), P("rcv"), P())
    out_specs = (P(None, None, "rcv", "src"), P(None, None, "rcv", "src"))
    return jax.shard_map(
        per_device, mesh=mesh, in_specs=in_specs, out_specs=out_specs, check_vma=False
    )
```

```python
import functools

import jax
import jax.numpy as jnp
from jax import lax
from jax.experimental import pallas as pl
from jax.experimental.pallas import tpu as pltpu
from jax.sharding import PartitionSpec as P

APER = 64
SHIFT = 16
BLOCK = 64
HALF = BLOCK // 2
SHALF = 2
LANES = 128
DEPTH = 128
HALO = APER // 2 + SHIFT
FIRST = 2
GROUPS = 2
STRIP = 16
SLOTS = 8
MESH = pl.DeviceIdType.MESH


def split(cells):
    high = cells.astype(jnp.bfloat16)
    low = (cells - high.astype(jnp.float32)).astype(jnp.bfloat16)
    return high, low


def forward_kernel(axes, shift_hbm, taper_hbm, live_hbm, wave_hbm, band_hbm, *refs):
    wave_ref, mult_ref, gain_ref = refs[:3]
    (
        shift_ref, taper_ref, live_ref, mask_ref, band_ref, turn_ref,
        even_weight, odd_weight, even_high, odd_high, even_low, odd_low, above_ref, below_ref, edge_ref, next_ref, prev_ref, ends_ref, corner_ref, masks_ref, line_ref, came_ref,
        data_ref, inner_ref, outer_ref, mine_ref, plane_ref, space_ref,
        load_sem, small_sem, send_up, recv_up, send_down, recv_down, send_mask, recv_mask,
        send_edge, recv_edge, send_corner, recv_corner, send_a, recv_a, send_b, recv_b, flood_sem,
    ) = refs[3:]
    (slow, slow_count), (fast, fast_count) = axes
    slow_me, fast_me = lax.axis_index(slow), lax.axis_index(fast)
    _, slices, receivers, shots = wave_ref.shape
    blocks, group = receivers // BLOCK, slices // GROUPS
    share = 4 * group
    quarters = LANES // share
    has_above, has_below = fast_me > 0, fast_me < fast_count - 1
    has_prev, has_next = slow_me > 0, slow_me < slow_count - 1
    direct = slow_count * fast_count <= 32

    def peer_of(a, b):
        return {slow: lax.rem(slow_me + a, slow_count), fast: lax.rem(fast_me + b, fast_count)}

    corners = []
    for i, (down, right) in enumerate([(1, 1), (1, -1), (-1, 1), (-1, -1)]):
        there = (has_below if down > 0 else has_above) & (has_next if right > 0 else has_prev)
        came = (has_above if down > 0 else has_below) & (has_prev if right > 0 else has_next)
        corners.append((i, there, came, {fast: fast_me + down, slow: slow_me + right}, 0 if down > 0 else 1))

    spans = [(0, LANES), (shots - LANES, LANES), (LANES, shots - 2 * LANES)]
    spans = [pl.ds(start, count) for start, count in spans if count > 0]

    def load(f, part):
        cells = (slice(None), f, slice(None), spans[part])
        return pltpu.make_async_copy(wave_hbm.at[cells], wave_ref.at[cells], load_sem.at[part, f])

    def wait_rest(f):
        for part in range(2, len(spans)):
            load(f, part).wait()

    def up(f):
        return pltpu.make_async_remote_copy(
            src_ref=wave_hbm.at[:, f, pl.ds(receivers - HALO, HALO)], dst_ref=above_ref.at[f],
            send_sem=send_up.at[f], recv_sem=recv_up.at[f],
            device_id={fast: fast_me + 1}, device_id_type=MESH,
        )

    def down(f):
        return pltpu.make_async_remote_copy(
            src_ref=wave_hbm.at[:, f, pl.ds(0, HALO)], dst_ref=below_ref.at[f],
            send_sem=send_down.at[f], recv_sem=recv_down.at[f],
            device_id={fast: fast_me - 1}, device_id_type=MESH,
        )

    def mask_copy(i):
        return pltpu.make_async_remote_copy(
            src_ref=line_ref.at[i], dst_ref=came_ref.at[i],
            send_sem=send_mask.at[i], recv_sem=recv_mask.at[i],
            device_id={fast: fast_me - 1 if i else fast_me + 1}, device_id_type=MESH,
        )

    def edge_copy(g, i):
        return pltpu.make_async_remote_copy(
            src_ref=edge_ref.at[g, 1 - i], dst_ref=next_ref.at[g] if i else prev_ref.at[g],
            send_sem=send_edge.at[g, i], recv_sem=recv_edge.at[g, i],
            device_id={slow: slow_me - 1 if i else slow_me + 1}, device_id_type=MESH,
        )

    def corner_copy(i, peer, end):
        return pltpu.make_async_remote_copy(
            src_ref=ends_ref.at[end, 1 - i % 2], dst_ref=corner_ref.at[i],
            send_sem=send_corner.at[i], recv_sem=recv_corner.at[i],
            device_id=peer, device_id_type=MESH,
        )

    def send_halos(f):
        @pl.when(has_below)
        def _():
            up(f).start()

        @pl.when(has_above)
        def _():
            down(f).start()

    small = [
        pltpu.make_async_copy(a, b, small_sem.at[i])
        for i, (a, b) in enumerate(
            [(live_hbm, live_ref), (taper_hbm, taper_ref), (shift_hbm, shift_ref), (band_hbm, band_ref)]
        )
    ]
    for copy in small[:3]:
        copy.start()
    barrier = pltpu.get_barrier_semaphore()
    near = [
        (has_above, {fast: fast_me - 1}), (has_below, {fast: fast_me + 1}),
        (has_prev, {slow: slow_me - 1}), (has_next, {slow: slow_me + 1}),
    ]
    beside = sum(there.astype(jnp.int32) for there, _ in near)
    greeted = beside + sum(there.astype(jnp.int32) for _, there, *_ in corners)
    for there, peer in near + [(there, peer) for _, there, _, peer, _ in corners]:
        @pl.when(there)
        def _():
            pl.semaphore_signal(barrier, inc=1, device_id=peer, device_id_type=MESH)

    small[3].start()

    for parts in (range(2), range(2, len(spans))):
        @pl.loop(0, slices)
        def _(f):
            for part in parts:
                load(f, part).start()

    pl.semaphore_wait(barrier, greeted)

    for f in range(FIRST):
        send_halos(f)

    small[0].wait()
    line = lax.broadcasted_iota(jnp.int32, (8, LANES), 0)

    @pl.loop(0, receivers // 8, unroll=4)
    def _(i):
        cells = jnp.zeros((8, LANES), jnp.float32)
        for r in range(8):
            cells = jnp.where(line == r, live_ref[i * 8 + r].astype(jnp.float32), cells)
        mask_ref[pl.ds(pl.multiple_of(i * 8, 8), 8), :] = cells

    diagonal = lax.broadcasted_iota(jnp.int32, (HALO, LANES), 0) == lax.broadcasted_iota(jnp.int32, (HALO, LANES), 1)
    for i, start in enumerate((receivers - HALO, 0)):
        cells = jnp.where(diagonal, mask_ref[start : start + HALO, :], 0.0)
        line_ref[i] = jnp.sum(cells, axis=0, keepdims=True)

    @pl.when(has_below)
    def _():
        mask_copy(0).start()

    @pl.when(has_above)
    def _():
        mask_copy(1).start()

    small[1].wait()
    small[2].wait()

    source = lax.broadcasted_iota(jnp.int32, (2 * LANES, LANES), 0)
    source = jnp.where(source < LANES, source, jnp.where(source < LANES + LANES // 2, source, source - 2 * LANES))
    offset = source - lax.broadcasted_iota(jnp.int32, (2 * LANES, LANES), 1) + SHALF
    turn = jnp.zeros((2 * LANES, LANES), jnp.float32)
    for u in range(2 * SHALF + 1):
        turn = jnp.where(offset == u, taper_ref[u], turn)
    turn = jnp.concatenate(split(turn), axis=1)
    for i in range(2):
        turn_ref[2 * i * LANES : 2 * (i + 1) * LANES, :] = turn

    rows_refs, weight_refs = ((even_high, even_low), (odd_high, odd_low)), (even_weight, odd_weight)
    for there, ref in ((has_prev, prev_ref), (has_next, next_ref)):
        @pl.when(jnp.logical_not(there))
        def _():
            ref[...] = jnp.zeros_like(ref)

    for i, there, came, peer, end in corners:
        @pl.when(jnp.logical_not(came))
        def _():
            corner_ref[i] = jnp.zeros(corner_ref.shape[1:], jnp.float32)

    for i, (there, ref) in enumerate(((has_above, above_ref), (has_below, below_ref))):
        @pl.when(jnp.logical_not(there))
        def _():
            came_ref[i] = jnp.zeros(came_ref.shape[1:], jnp.float32)
            ref[0] = jnp.zeros(ref.shape[1:], jnp.float32)

    edge_ref[...] = jnp.zeros_like(edge_ref)

    column = lax.broadcasted_iota(jnp.int32, (BLOCK, LANES), 1)

    def prepare(f, odd):
        weight_ref = weight_refs[odd]
        live = (column // APER) == odd
        lanes = pl.ds(pl.multiple_of(f // 2 * LANES, LANES), LANES)
        for block in range(blocks):
            for x in range(2):
                cells = jnp.where(live, band_ref[x, block * BLOCK : (block + 1) * BLOCK, lanes], 0.0)
                cells = pltpu.roll(cells, shift_ref[block] + SHIFT + APER * odd, 1)
                for h in range(2):
                    taps = pltpu.roll(cells[h * HALF : (h + 1) * HALF], 0, 1, stride=1, stride_axis=0)
                    weight_ref[2 * block + h, 0, x], weight_ref[2 * block + h, 1, x] = split(taps)

    small[3].wait()
    prepare(0, 0)

    lane = lax.broadcasted_iota(jnp.int32, (BLOCK, LANES), 1)

    def packed(block):
        return pl.ds(block // quarters * BLOCK, BLOCK), block % quarters * share

    for g in range(GROUPS):
        @pl.loop(0, group, unroll=2)
        def _(i):
            f = g * group + i
            load(f, 0).wait()
            load(f, 1).wait()
            for chunk in range(0, blocks, quarters):
                rows, _ = packed(chunk)
                first, last = edge_ref[g, 0, rows, :], edge_ref[g, 1, rows, :]
                for block in range(chunk, min(chunk + quarters, blocks)):
                    cells = pl.ds(block * BLOCK, BLOCK)
                    for x in range(2):
                        place = packed(block)[1] + 4 * i + 2 * x
                        ours = (lane >= place) & (lane < place + 2)
                        first = jnp.where(ours, pltpu.roll(wave_ref[x, f, cells, :LANES], place, 1), first)
                        turned = pltpu.roll(wave_ref[x, f, cells, shots - LANES :], lax.rem(place + 2, LANES), 1)
                        last = jnp.where(ours, turned, last)
                edge_ref[g, 0, rows, :] = first
                edge_ref[g, 1, rows, :] = last

        @pl.when(has_next)
        def _():
            edge_copy(g, 0).start()

        @pl.when(has_prev)
        def _():
            edge_copy(g, 1).start()

    fold = HALO // 2
    wide = lax.broadcasted_iota(jnp.int32, (HALO, LANES), 1)
    for end, block, skip in ((0, blocks - 1, BLOCK - HALO), (1, 0, 0)):
        rows, place = packed(block)
        for side in range(2):
            cells = jnp.zeros((HALO, LANES), jnp.float32)
            for g in range(GROUPS):
                part = pltpu.roll(edge_ref[g, side, rows, :][skip : skip + HALO], (g * share - place) % LANES, 1)
                cells = jnp.where((wide >= g * share) & (wide < (g + 1) * share), part, cells)
            ends_ref[end, side] = jnp.where(
                wide[:fold] < LANES // 2, cells[:fold], pltpu.roll(cells[fold:], LANES // 2, 1)
            )

    for i, there, came, peer, end in corners:
        @pl.when(there)
        def _():
            corner_copy(i, peer, end).start()

    @pl.loop(FIRST, slices)
    def _(f):
        send_halos(f)

    def turned(after, before, at_after, at_before):
        count = after.shape[0]
        after = pltpu.roll(after, lax.rem(LANES - at_after, LANES), 1)
        before = pltpu.roll(before, lax.rem(2 * LANES - 2 - at_before, LANES), 1)
        return jnp.where(lax.broadcasted_iota(jnp.int32, (count, LANES), 1) < LANES // 2, after, before)

    def stage(odd, x, wave, mask, outside, at):
        high_ref, low_ref = rows_refs[odd]
        count = wave.shape[0]
        tile = lax.broadcasted_iota(jnp.int32, (count, LANES), 1) < LANES // 2
        outside = split(outside * mask)
        inside = [split(wave[:, i * LANES : (i + 1) * LANES] * mask) for i in range(shots // LANES)]
        cells = [outside, *inside, outside]
        parts = []
        for part in range(2):
            rows = []
            for i in range(shots // LANES):
                around = jnp.where(tile, cells[i + 2][part], cells[i][part])
                rows.append(jnp.concatenate([cells[i + 1][part], around], axis=1))
            parts.append(jnp.concatenate(rows, axis=0))
        both = jnp.dot(jnp.concatenate(parts, axis=1), turn_ref[...], preferred_element_type=jnp.float32)
        high, low = split(both[:, :LANES] + both[:, LANES:])
        rows = pl.ds(at, count)
        for i in range(shots // LANES):
            lanes = pl.ds(i * LANES, LANES)
            high_ref[x, rows, lanes] = high[i * count : (i + 1) * count]
            low_ref[x, rows, lanes] = low[i * count : (i + 1) * count]

    def predict(f, odd, block):
        (high_ref, low_ref), weight_ref = rows_refs[odd], weight_refs[odd]
        total = jnp.zeros((8, shots), jnp.float32)
        for h in range(2):
            half = 2 * block + h
            base = half * HALF
            parts = []
            for part in range(2):
                real, imag = weight_ref[half, part, 0], weight_ref[half, part, 1]
                parts.append(jnp.concatenate([real, -imag], axis=1))
                parts.append(jnp.concatenate([imag, real], axis=1))
            window = pl.ds(base, DEPTH)
            high = jnp.concatenate([high_ref[x, window, :] for x in range(2)], axis=0)
            low = jnp.concatenate([low_ref[x, window, :] for x in range(2)], axis=0)
            upper = jnp.dot(jnp.concatenate(parts, axis=0), high, preferred_element_type=jnp.float32)
            lower = jnp.dot(jnp.concatenate(parts[:2], axis=0), low, preferred_element_type=jnp.float32)
            pred = upper[:BLOCK] + (upper[BLOCK:] + lower)
            for x in range(2):
                mult_ref[x, f, pl.ds(base, HALF), :] = pred[x * HALF : (x + 1) * HALF]
            total = total + jnp.sum((pred * pred).reshape(-1, 8, shots), axis=0)
        return total

    def lanes_of(total):
        return sum(total[:, i * LANES : (i + 1) * LANES] for i in range(shots // LANES))

    def wait_edges(g):
        @pl.when(has_prev)
        def _():
            edge_copy(g, 0).wait_recv()

        @pl.when(has_next)
        def _():
            edge_copy(g, 1).wait_recv()

    def wait_halos(f, sides=(0, 1)):
        for side in sides:
            @pl.when(has_below if side else has_above)
            def _():
                (down if side else up)(f).wait_recv()

    def stage_own(f, odd):
        g, i = f // group, lax.rem(f, group)
        data = jnp.zeros((8, LANES), jnp.float32)
        for block in range(blocks):
            rows = pl.ds(block * BLOCK, BLOCK)
            cells, place = packed(block)
            after, before = next_ref[g, cells, :], prev_ref[g, cells, :]
            for x in range(2):
                wave = wave_ref[x, f, rows, :]
                at = place + 4 * i + 2 * x
                stage(odd, x, wave, mask_ref[rows, :], turned(after, before, at, at), block * BLOCK + HALO)
                data = data + lanes_of(jnp.sum((wave * wave).reshape(-1, 8, shots), axis=0))
        data_ref[f] = data

    def stage_halos(f, odd, sides=(0, 1)):
        for x in range(2):
            at = 4 * f + 2 * x
            for k in sides:
                ref, start, there = ((above_ref, 0, has_above), (below_ref, HALO + receivers, has_below))[k]
                ends = [turned(corner_ref[2 * k + 1], corner_ref[2 * k], at + c, at + c) for c in (0, LANES // 2)]
                outside = jnp.concatenate(ends, axis=0)
                stage(odd, x, ref[f * there.astype(jnp.int32), x], masks_ref[k], outside, start)

    def predict_inner(f, odd):
        total = jnp.zeros((8, shots), jnp.float32)
        for block in range(1, blocks - 1):
            total = total + predict(f, odd, block)
        inner_ref[f] = lanes_of(total)

    def predict_outer(f, odd):
        total = jnp.zeros((8, shots), jnp.float32)
        for block in sorted({0, blocks - 1}):
            total = total + predict(f, odd, block)
        outer_ref[f] = lanes_of(total)

    def flood(n):
        for there, peer in near:
            @pl.when(there)
            def _():
                pl.semaphore_signal(flood_sem.at[n], inc=1, device_id=peer, device_id_type=MESH)

    def step(f, odd):
        @pl.when(f > 0)
        def _():
            pl.semaphore_wait(flood_sem.at[f - 1], beside)

        flood(f)
        wait_rest(f + 1)
        wait_halos(f)
        stage_halos(f, odd)
        stage_own(f + 1, 1 - odd)
        predict_outer(f, odd)
        predict_inner(f + 1, 1 - odd)

    wait_edges(0)
    wait_rest(0)
    stage_own(0, 0)
    prepare(1, 1)
    predict_inner(0, 0)

    @pl.when(has_above)
    def _():
        mask_copy(0).wait_recv()

    @pl.when(has_below)
    def _():
        mask_copy(1).wait_recv()

    for i, there, came, peer, end in corners:
        @pl.when(came)
        def _():
            corner_copy(i, peer, end).wait_recv()

    for i in range(2):
        cells = jnp.sum(jnp.where(diagonal, came_ref[i], 0.0), axis=1, keepdims=True)
        masks_ref[i] = jnp.broadcast_to(cells, masks_ref.shape[1:])

    @pl.loop(0, slices // 2 - 1)
    def _(pair):
        f = 2 * pair
        step(f, 0)
        prepare(f + 2, 0)
        for g in range(1, GROUPS):
            @pl.when(f + 2 == g * group)
            def _():
                wait_edges(g)

        step(f + 1, 1)
        prepare(f + 3, 1)

    step(slices - 2, 0)
    pl.semaphore_wait(flood_sem.at[slices - 2], beside)

    last = slices - 1
    outer_ref[last] = jnp.zeros((8, LANES), jnp.float32)
    cells = jnp.concatenate([jnp.sum(data_ref[...], axis=1), jnp.sum(inner_ref[...] + outer_ref[...], axis=1)], axis=0)
    row = lax.broadcasted_iota(jnp.int32, cells.shape, 0)
    col = lax.broadcasted_iota(jnp.int32, cells.shape, 1)
    spot = jnp.where(row < slices, row, row - slices + LANES // 2)
    cells = jnp.where(col == spot, jnp.sum(cells, axis=1, keepdims=True), 0.0)
    mine_ref[...] = jnp.sum(cells, axis=0, keepdims=True)

    if blocks > 1:
        for parity, sides in ((0, (1, 0)), (1, (0, 1))):
            @pl.when(lax.rem(fast_me, 2) == parity)
            def _():
                for side in sides:
                    wait_halos(last, (side,))
                    stage_halos(last, 1, (side,))
                    outer_ref[last] += lanes_of(predict(last, 1, (blocks - 1) * side))
    else:
        wait_halos(last)
        stage_halos(last, 1)
        predict_outer(last, 1)
    for n in range(slices - 1, flood_sem.shape[0]):
        flood(n)
        pl.semaphore_wait(flood_sem.at[n], beside)

    tail = jnp.sum(jnp.sum(outer_ref[last], axis=0, keepdims=True), axis=1, keepdims=True)
    spot = lax.broadcasted_iota(jnp.int32, (1, LANES), 1) == LANES // 2 + last
    mine = mine_ref[...] + jnp.where(spot, tail, 0.0)
    mine_ref[...] = mine

    def exchange(source, target, pairs, send, recv):
        copies = []
        for n, (a, b) in enumerate(pairs):
            copy = pltpu.make_async_remote_copy(
                src_ref=source, dst_ref=target.at[n], send_sem=send.at[n], recv_sem=recv.at[n],
                device_id=peer_of(a, b), device_id_type=MESH,
            )
            copy.start()
            copies.append(copy)
        for copy in copies:
            copy.wait()

    if direct:
        pairs = [(a, b) for b in range(fast_count) for a in range(slow_count) if a or b]
        pairs.sort(key=lambda pair: min(pair[1], fast_count - pair[1]) or fast_count)
        exchange(mine_ref, space_ref, pairs, send_b, recv_b)
        total = mine + jnp.sum(space_ref[...], axis=0)
    else:
        exchange(mine_ref, plane_ref, [(a, 0) for a in range(1, slow_count)], send_a, recv_a)
        total = mine + jnp.sum(plane_ref[...], axis=0)
        mine_ref[...] = total
        exchange(mine_ref, space_ref, [(0, b) for b in range(1, fast_count)], send_b, recv_b)
        total = total + jnp.sum(space_ref[...], axis=0)
    gain_ref[...] = jnp.sqrt((total + 1e-06) / (pltpu.roll(total, LANES // 2, 1) + 1e-06))

    @pl.when(has_below)
    def _():
        mask_copy(0).wait_send()

        @pl.loop(0, slices)
        def _(f):
            up(f).wait_send()

    @pl.when(has_above)
    def _():
        mask_copy(1).wait_send()

        @pl.loop(0, slices)
        def _(f):
            down(f).wait_send()

    for g in range(GROUPS):
        @pl.when(has_next)
        def _():
            edge_copy(g, 0).wait_send()

        @pl.when(has_prev)
        def _():
            edge_copy(g, 1).wait_send()

    for i, there, came, peer, end in corners:
        @pl.when(there)
        def _():
            corner_copy(i, peer, end).wait_send()


def forward(axes, wave, band, shift, live, taper):
    _, slices, receivers, shots = wave.shape
    slow_count, fast_count = axes[0][1], axes[1][1]
    direct = slow_count * fast_count <= 32
    peers = slow_count * fast_count - 1 if direct else fast_count - 1
    farthest = slow_count + fast_count - 2 if direct else max(slow_count, fast_count) - 1
    tall = receivers + DEPTH - HALF
    blocks, quarters = receivers // BLOCK, LANES // (4 * slices // GROUPS)
    packed = -(-blocks // quarters) * BLOCK
    dma = pltpu.SemaphoreType.DMA
    whole = pl.BlockSpec(memory_space=pltpu.VMEM)
    hbm = pl.BlockSpec(memory_space=pltpu.HBM)
    return pl.pallas_call(
        functools.partial(forward_kernel, axes),
        in_specs=[hbm] * 5,
        out_specs=[whole, whole, whole],
        out_shape=[
            jax.ShapeDtypeStruct(wave.shape, jnp.float32),
            jax.ShapeDtypeStruct(wave.shape, jnp.float32),
            jax.ShapeDtypeStruct((1, LANES), jnp.float32),
        ],
        scratch_shapes=[
            pltpu.SMEM(shift.shape, jnp.int32),
            pltpu.SMEM(taper.shape, jnp.float32),
            pltpu.SMEM(live.shape, jnp.int32),
            pltpu.VMEM((receivers, LANES), jnp.float32),
            pltpu.VMEM(band.shape, jnp.float32),
            pltpu.VMEM((4 * LANES, 2 * LANES), jnp.bfloat16),
            *[pltpu.VMEM((receivers // HALF, 2, 2, HALF, DEPTH), jnp.bfloat16)] * 2,
            *[pltpu.VMEM((2, tall, shots), jnp.bfloat16)] * 4,
            pltpu.VMEM((slices, 2, HALO, shots), jnp.float32),
            pltpu.VMEM((slices, 2, HALO, shots), jnp.float32),
            pltpu.VMEM((GROUPS, 2, packed, LANES), jnp.float32),
            pltpu.VMEM((GROUPS, packed, LANES), jnp.float32),
            pltpu.VMEM((GROUPS, packed, LANES), jnp.float32),
            pltpu.VMEM((2, 2, HALO // 2, LANES), jnp.float32),
            pltpu.VMEM((4, HALO // 2, LANES), jnp.float32),
            pltpu.VMEM((2, HALO, LANES), jnp.float32),
            pltpu.VMEM((2, 1, LANES), jnp.float32),
            pltpu.VMEM((2, 1, LANES), jnp.float32),
            *[pltpu.VMEM((slices, 8, LANES), jnp.float32)] * 3,
            pltpu.VMEM((1, LANES), jnp.float32),
            pltpu.VMEM((slow_count - 1, 1, LANES), jnp.float32),
            pltpu.VMEM((peers, 1, LANES), jnp.float32),
            dma((3, slices)), dma((4,)), dma((slices,)), dma((slices,)), dma((slices,)), dma((slices,)),
            dma((2,)), dma((2,)), dma((GROUPS, 2)), dma((GROUPS, 2)), dma((4,)), dma((4,)),
            dma((slow_count - 1,)), dma((slow_count - 1,)), dma((peers,)), dma((peers,)),
            pltpu.SemaphoreType.REGULAR((max(slices, farthest) - 1,)),
        ],
        cost_estimate=pl.CostEstimate(flops=2**33, bytes_accessed=wave.size * 8, transcendentals=0),
        compiler_params=pltpu.CompilerParams(
            collective_id=1, has_side_effects=True, vmem_limit_bytes=14 * 2**20
        ),
        name="forward",
    )(shift, taper, live, wave, band)


def finish_kernel(gain_ref, wave_ref, mult_ref, mult_hbm, prim_hbm, prim_ref, mult_sem, prim_sem):
    slices = wave_ref.shape[1]
    slots = prim_ref.shape[0]

    def mult_copy(f):
        return pltpu.make_async_copy(mult_ref.at[:, f], mult_hbm.at[:, f], mult_sem.at[f])

    def prim_copy(f):
        return pltpu.make_async_copy(prim_ref.at[lax.rem(f, slots)], prim_hbm.at[:, f], prim_sem.at[f])

    col = lax.broadcasted_iota(jnp.int32, (1, LANES), 1)

    @pl.loop(0, slices)
    def _(f):
        mult_copy(f).start()
        gain = jnp.sum(jnp.where(col == f, gain_ref[...], 0.0))

        @pl.when(f >= slots)
        def _():
            prim_copy(f - slots).wait()

        for x in range(2):
            for r in range(0, wave_ref.shape[2], BLOCK):
                rows = pl.ds(r, BLOCK)
                prim_ref[lax.rem(f, slots), x, rows, :] = wave_ref[x, f, rows, :] - gain * mult_ref[x, f, rows, :]
        prim_copy(f).start()

    @pl.loop(0, slices)
    def _(f):
        mult_copy(f).wait()

    @pl.loop(max(slices - slots, 0), slices)
    def _(f):
        prim_copy(f).wait()


def finish(gain, wave, mult):
    slices = wave.shape[1]
    whole = pl.BlockSpec(memory_space=pltpu.VMEM)
    hbm = pl.BlockSpec(memory_space=pl.ANY)
    return pl.pallas_call(
        finish_kernel,
        in_specs=[whole, whole, whole],
        out_specs=[hbm, hbm],
        out_shape=[jax.ShapeDtypeStruct(wave.shape, jnp.float32)] * 2,
        scratch_shapes=[
            pltpu.VMEM((min(SLOTS, slices), 2, *wave.shape[2:]), jnp.float32),
            pltpu.SemaphoreType.DMA((slices,)),
            pltpu.SemaphoreType.DMA((slices,)),
        ],
        cost_estimate=pl.CostEstimate(flops=wave.size * 2, bytes_accessed=wave.size * 8, transcendentals=0),
        compiler_params=pltpu.CompilerParams(vmem_limit_bytes=12 * 2**20),
        name="finish",
    )(gain, wave, mult)


def per_device(wavefield, surface_band, band_shift, trace_mask, shot_taper):
    axes = (("src", lax.axis_size("src")), ("rcv", lax.axis_size("rcv")))
    def keep(array):
        return pltpu.with_memory_space_constraint(array, pltpu.HBM) if array.size > 1 else array

    small = [keep(array) for array in (surface_band, band_shift, trace_mask, shot_taper)]
    wave, mult, gain = forward(axes, wavefield, *small)
    return tuple(finish(gain, wave, mult))


def solution(mesh):
    in_specs = (P(None, None, "rcv", "src"), P(None, "rcv", None), P("rcv"), P("rcv"), P())
    out_specs = (P(None, None, "rcv", "src"), P(None, None, "rcv", "src"))
    return jax.shard_map(
        per_device, mesh=mesh, in_specs=in_specs, out_specs=out_specs, check_vma=False
    )
```
